256 devices in a mesh: outer: 8 (over z), inner: 32 (over x, y, core).
Axes of the slice: x: 4, y: 4, z: 8, core: 2. Of those that a mesh axis runs over, the one named last changes fastest.
Arguments:
- normals: bfloat16 [1024, 512, 512], P('outer', 'inner'), may hold values from -6 to 6
- states: bfloat16 [1024, 512], P('outer'), may hold values from -0.29882812 to 0.29882812
- loadings: bfloat16 [2048, 512], replicated, may hold values from -6 to 6
- strikes: float32 [2048], replicated, may hold values from -6 to 6
- hedge: float32 [2048], replicated, may hold values from -384 to 384
- sigma: float32 [512], replicated, may hold values from 0.02 to 0.1
- tail: int32 [256], replicated, may hold values from 0 to 1023, as said below
Outputs:
- grad: float32 [2048, 512], P(('outer', 'inner'))
The draws below stay inside these ranges and needn't reach their ends.
Inputs may be any that keep to these rules, and one draw needn't show every extreme that they name: Increasing and distinct. Group g holds nodes g * 128 to (g + 1) * 128 - 1; at most 80 tail indices fall into one group, and some group holds exactly 80.
All inputs are finite; a program needn't handle non-finite values.
Results may differ from the reference program's by a relative error of at most 0.00057.
Values may be sent and summed in bfloat16 or wider, within the bound.
A program may use at most 64 MiB of HBM per device.

```python
import math
import jax
import jax.numpy as jnp
from jax import lax

M = 2048
K = 512
GROUPS = 8
PATHS = 512
NODE_GRP = 128
NODES = 1024
TAIL = 256
CAP = 80


def draw_tail(key, part):
    first_key, second_key, third_key = jax.random.split(jax.random.fold_in(key, 17), 3)
    heavy = jax.random.randint(first_key, (), 0, GROUPS)
    groups_idx = jnp.arange(GROUPS, dtype=jnp.int32)
    others = GROUPS - 1
    rank = (groups_idx - heavy - 1) % GROUPS
    remain = TAIL - CAP
    base = remain // others
    extra = remain % others
    drawn = base + (rank < extra).astype(jnp.int32)
    shifts = jax.random.randint(second_key, (GROUPS,), 0, base // 2 + 1)
    shifts = jnp.where(rank == others, 0, shifts)
    before = (heavy + 1 + (rank - 1) % others) % GROUPS
    counts = jnp.where(rank == others, CAP, drawn + shifts - shifts[before])
    offsets = jax.random.randint(third_key, (GROUPS,), 0, NODE_GRP - counts + 1)
    ends = jnp.cumsum(counts)
    begins = ends - counts
    places = jnp.arange(TAIL, dtype=jnp.int32)
    owner = jnp.sum((places[:, None] >= ends[None, :]).astype(jnp.int32), axis=1)
    return (owner * NODE_GRP + offsets[owner] + places - begins[owner]).astype(jnp.int32)


def level_of(stream_key, shape, shards, low, top_value):
    factor_of, own = 1.0, jax.random.fold_in(stream_key, 6)
    for position, shards_of in shards:
        heights = jnp.exp(jax.random.uniform(jax.random.fold_in(own, position), (shards_of,), jnp.float32, low / len(shards), top_value / len(shards)))
        factor_of = factor_of * jnp.repeat(heights, shape[position] // shards_of).reshape([-1 if axis == position else 1 for axis in range(len(shape))])
    return factor_of


def gaussian(own_key, dims, deviation, bound, shards=(), held_as=jnp.bfloat16):
    factor_of = level_of(own_key, dims, shards, -0.22, 0.18) if shards else 1.0
    entries = jax.random.normal(own_key, dims, jnp.float32) * deviation * factor_of
    return jnp.minimum(jnp.maximum(entries, -bound), bound).astype(held_as)


def setup_inputs(seed: int = 0) -> dict:
    key_of = jax.random.split(jax.random.key(seed), 8)
    normals = gaussian(key_of[0], (NODES, PATHS, K), 1.0, 6.0, ((0, 8), (1, 32)))
    states = gaussian(key_of[1], (NODES, K), 0.05, 0.29882812, ((0, 8),))
    loadings = gaussian(key_of[2], (M, K), 1.0, 6.0)
    strikes = gaussian(key_of[3], (M,), 1.0, 6.0, (), jnp.float32)
    hedge = gaussian(key_of[4], (M,), 64.0, 384.0, (), jnp.float32)
    sigma = jnp.clip(jnp.exp(jax.random.uniform(key_of[5], (K,), jnp.float32, math.log(0.02), math.log(0.1))), 0.02, 0.1)
    tail = draw_tail(jax.random.fold_in(key_of[7], 71), 0)
    return {"normals": normals, "states": states, "loadings": loadings, "strikes": strikes, "hedge": hedge, "sigma": sigma, "tail": tail}


EPSILON = 1e-06

def reference(normals, states, loadings, strikes, hedge, sigma, tail):
    width = math.gcd(TAIL, 8)
    starts = jnp.arange(0, TAIL, width).astype(jnp.int32)

    def block(total, start):
        nodes = lax.dynamic_slice_in_dim(tail, start, width, 0)
        values = jnp.take(normals, nodes, axis=0).astype(jnp.float32)
        center = lax.optimization_barrier(jnp.sum(values, axis=1)) / PATHS
        spread = lax.optimization_barrier(jnp.sum(values * values, axis=1)) / PATHS - center * center
        scaled = ((values - center[:, None, :]) * lax.rsqrt(spread + EPSILON)[:, None, :]).astype(jnp.bfloat16)
        levels = jnp.take(states, nodes, axis=0).astype(jnp.float32)
        factors = (levels[:, None, :] + sigma * scaled.astype(jnp.float32)).astype(jnp.bfloat16)
        factors = factors.reshape(width * PATHS, K)
        level = lax.dot_general(factors, loadings, (((1,), (1,)), ((), ())), preferred_element_type=jnp.float32) - strikes
        weight = (hedge * jax.nn.sigmoid(level)).astype(jnp.bfloat16)
        cross = lax.dot_general(weight, scaled.reshape(width * PATHS, K), (((0,), (0,)), ((), ())), preferred_element_type=jnp.float32)
        return (total + cross, None)
    total, unused = lax.scan(block, jnp.zeros((M, K), jnp.float32), starts)
    return loadings.astype(jnp.float32) * total / (TAIL * PATHS)
```

```python
import jax
import jax.numpy as jnp
from jax import lax
from jax.experimental import pallas as pl
from jax.experimental.pallas import tpu as pltpu
from jax.sharding import PartitionSpec as P

CAP = 80
EPSILON = 1e-06
CHUNKS = 4
BLOCKS = 5
MESH = pl.DeviceIdType.MESH
F32 = jnp.float32
BF16 = jnp.bfloat16


def place(hit):
    return jnp.where(hit, 1.0, 0.0)


def kernel(
    normals, states, loadings, strikes, hedge, sigma, tail, out,
    own, pair, load_v, states_b, states_f, strikes_v, hedge_v, sigma_v, tail_s, slot_s, live_s,
    sums, sums_in, stat, stats, half_strike, half_hedge, own_load, load_t,
    mixed, part, turned, weight, acc, sent, in_x, in_y, mid_x, mid_y, in_xy, in_yx, last, in_z,
    copy_sem, pair_sem, sum_out, sum_in, stat_out, stat_in,
    x_out, x_in, y_out, y_in, xy_out, xy_in, yx_out, yx_in, z_out, z_in,
):
    z = lax.axis_index("outer")
    me = lax.axis_index("inner")
    x, y, c = me // 8, (me // 2) % 4, me % 2
    nodes, per_node, factors = own.shape
    paths = per_node * 32
    tails = tail_s.shape[0]

    loads = [
        pltpu.make_async_copy(tail, tail_s, copy_sem.at[0]),
        pltpu.make_async_copy(normals, own, copy_sem.at[1]),
        pltpu.make_async_copy(states, states_b, copy_sem.at[2]),
        pltpu.make_async_copy(sigma, sigma_v, copy_sem.at[3]),
        pltpu.make_async_copy(strikes, strikes_v, copy_sem.at[4]),
        pltpu.make_async_copy(hedge, hedge_v, copy_sem.at[5]),
        pltpu.make_async_copy(loadings, load_v, copy_sem.at[6]),
    ]
    for item in loads:
        item.start()

    barrier = pltpu.get_barrier_semaphore()

    def greet_plane(r, carry):
        pl.semaphore_signal(
            barrier, inc=1, device_id=(z, (me + r) % 32), device_id_type=MESH
        )
        return carry

    def greet_line(r, carry):
        pl.semaphore_signal(
            barrier, inc=1, device_id=((z + r) % 8, me), device_id_type=MESH
        )
        return carry

    lax.fori_loop(1, 32, greet_plane, 0)
    lax.fori_loop(1, 8, greet_line, 0)

    loads[0].wait()
    first = jnp.int32(0)
    step = tails // 2
    while step:
        first = first + jnp.where(tail_s[first + step - 1] < z * nodes, step, 0)
        step //= 2

    def find(s, carry):
        at = jnp.minimum(first + s, tails - 1)
        node = tail_s[at] - z * nodes
        good = (first + s < tails) & (node >= 0) & (node < nodes)
        slot_s[s] = jnp.clip(node, 0, nodes - 1)
        live_s[s] = jnp.where(good, 1.0, 0.0).astype(F32)
        return carry

    lax.fori_loop(0, CAP, find, 0)
    loads[1].wait()

    def add_up(q, carry):
        for i in range(5):
            block = own[slot_s[q * 5 + i]].astype(F32)
            one = jnp.sum(block, axis=0, keepdims=True)
            two = jnp.sum(block * block, axis=0, keepdims=True)
            for h in range(2):
                for b in range(2):
                    lanes = slice(h * 256 + b * 128, h * 256 + b * 128 + 128)
                    sums[q * 2 + h, i, b : b + 1, :] = one[:, lanes]
                    sums[q * 2 + h, i, 2 + b : 3 + b, :] = two[:, lanes]
        return carry

    lax.fori_loop(0, 16, add_up, 0)
    pl.semaphore_wait(barrier, 38)

    def sum_copy(r, owner, source):
        return pltpu.make_async_remote_copy(
            src_ref=sums.at[owner], dst_ref=sums_in.at[source],
            send_sem=sum_out.at[r], recv_sem=sum_in.at[r],
            device_id=(z, owner), device_id_type=MESH,
        )

    def send_sums(r, carry):
        sum_copy(r, (me + r) % 32, me).start()
        return carry

    lax.fori_loop(1, 32, send_sums, 0)
    swap = pltpu.make_async_remote_copy(
        src_ref=own, dst_ref=pair, send_sem=pair_sem.at[0], recv_sem=pair_sem.at[1],
        device_id=(z, me + 1 - 2 * c), device_id_type=MESH,
    )
    swap.start()

    for item in loads[2:]:
        item.wait()
    states_f[...] = states_b[...].astype(F32)
    m_id = lax.broadcasted_iota(jnp.int32, (256, 256), 0)
    l_id = lax.broadcasted_iota(jnp.int32, (256, 256), 1)
    same = (m_id // 16 == l_id // 16) & (m_id % 8 == l_id % 8)
    picks = [same & ((m_id // 8) % 2 == c) & ((l_id // 8) % 2 == a) for a in range(2)]
    same_t = (m_id // 16 == l_id // 16) & (m_id % 8 == l_id % 8)
    picks_t = [same_t & ((l_id // 8) % 2 == c) & ((m_id // 8) % 2 == a) for a in range(2)]
    for source, target in ((strikes_v, half_strike), (hedge_v, half_hedge)):
        rows = source[...] * 0.5
        moved = [
            jnp.dot(rows, place(pick), precision=lax.Precision.HIGHEST, preferred_element_type=F32)
            for pick in picks
        ]
        for j in range(CHUNKS):
            target[j] = moved[0][2 * j : 2 * j + 1] + moved[1][2 * j + 1 : 2 * j + 2]
    turn = [place(pick).astype(BF16) for pick in picks_t]

    def order(j, carry):
        rows = jnp.zeros((256, factors), F32)
        for a in range(2):
            at = pl.multiple_of((2 * j + a) * 256, 256)
            rows = rows + jnp.dot(turn[a], load_v[pl.ds(at, 256), :], preferred_element_type=F32)
        own_load[j] = rows
        load_t[j] = (rows * 0.5).astype(BF16).T
        return carry

    lax.fori_loop(0, CHUNKS, order, 0)

    def wait_sums(r, carry):
        sum_copy(r, me, (me + 32 - r) % 32).wait_recv()
        return carry

    lax.fori_loop(1, 32, wait_sums, 0)

    def gather_sums(r, total):
        return total + sums_in[(me + r) % 32]

    total = lax.fori_loop(1, 32, gather_sums, sums[me])
    center = total[:, 0:2, :] / paths
    spread = total[:, 2:4, :] / paths - center * center
    stat[:, 0:2, :] = center
    stat[:, 2:4, :] = lax.rsqrt(spread + EPSILON)
    stats[me] = stat[...]

    def stat_copy(r, target, source):
        return pltpu.make_async_remote_copy(
            src_ref=stat, dst_ref=stats.at[source],
            send_sem=stat_out.at[r], recv_sem=stat_in.at[r],
            device_id=(z, target), device_id_type=MESH,
        )

    def send_stats(r, carry):
        stat_copy(r, (me + r) % 32, me).start()
        return carry

    lax.fori_loop(1, 32, send_stats, 0)
    swap.wait_recv()

    def wait_stats(r, carry):
        stat_copy(r, me, (me + 32 - r) % 32).wait_recv()
        return carry

    lax.fori_loop(1, 32, wait_stats, 0)

    def normalise(blk, carry):
        for u in range(4):
            s = blk * 4 + u
            q, i = s // 5, s % 5
            at, live = slot_s[s], live_s[s]
            state = states_f[pl.ds(at, 1), :]
            for e, source in enumerate((own, pair)):
                block = source[at]
                row = pl.multiple_of(s * 32 + e * 16, 16)
                for lane in range(4):
                    h, b = lane // 2, lane % 2
                    lanes = slice(lane * 128, lane * 128 + 128)
                    mean = stats[q * 2 + h, i, b : b + 1, :]
                    scale = stats[q * 2 + h, i, 2 + b : 3 + b, :] * live
                    scaled = ((block[:, lanes].astype(F32) - mean) * scale).astype(BF16)
                    both = state[:, lanes] + sigma_v[:, lanes] * scaled.astype(F32)
                    mixed[pl.ds(row, 16), lanes] = both.astype(BF16)
                    part[u * 32 + e * 16 : u * 32 + e * 16 + 16, lanes] = scaled
        at = pl.multiple_of((blk % 4) * 128, 128)
        turned[blk // 4, :, pl.ds(at, 128)] = part[...].T
        return carry

    lax.fori_loop(0, CAP // 4, normalise, 0)

    def weigh(j, b):
        at = b * 512 if isinstance(b, int) else pl.multiple_of(b * 512, 512)
        level = jnp.dot(mixed[pl.ds(at, 512), :], load_t[j], preferred_element_type=F32)
        size = half_hedge[j]
        return (size + size * jnp.tanh(level - half_strike[j])).astype(BF16)

    def cross(b, slot):
        return jnp.dot(turned[b], weight[slot], preferred_element_type=F32)

    def x_copy(j, r):
        px = (x + r) % 4
        return pltpu.make_async_remote_copy(
            src_ref=sent.at[j, px, :, :, pl.ds(0, 256)], dst_ref=in_x.at[j, r - 1],
            send_sem=x_out.at[j, r - 1], recv_sem=x_in.at[j, r - 1],
            device_id=(z, (px * 4 + y) * 2 + c), device_id_type=MESH,
        )

    def y_copy(j, r):
        py = (y + r) % 4
        return pltpu.make_async_remote_copy(
            src_ref=sent.at[j, :, py, :, pl.ds(256, 256)], dst_ref=in_y.at[j, r - 1],
            send_sem=y_out.at[j, r - 1], recv_sem=y_in.at[j, r - 1],
            device_id=(z, (x * 4 + py) * 2 + c), device_id_type=MESH,
        )

    def xy_copy(j, r):
        py = (y + r) % 4
        return pltpu.make_async_remote_copy(
            src_ref=mid_x.at[j, py], dst_ref=in_xy.at[j, r - 1],
            send_sem=xy_out.at[j, r - 1], recv_sem=xy_in.at[j, r - 1],
            device_id=(z, (x * 4 + py) * 2 + c), device_id_type=MESH,
        )

    def yx_copy(j, r):
        px = (x + r) % 4
        return pltpu.make_async_remote_copy(
            src_ref=mid_y.at[j, px], dst_ref=in_yx.at[j, r - 1],
            send_sem=yx_out.at[j, r - 1], recv_sem=yx_in.at[j, r - 1],
            device_id=(z, (px * 4 + y) * 2 + c), device_id_type=MESH,
        )

    def z_copy(j, a, slot):
        return pltpu.make_async_remote_copy(
            src_ref=last.at[j, a], dst_ref=in_z.at[slot],
            send_sem=z_out.at[j, a], recv_sem=z_in.at[slot],
            device_id=(2 * j + a, me), device_id_type=MESH,
        )

    def finish(j):
        rows = acc[...].astype(BF16).T
        sent[j] = rows.reshape(4, 4, 16, factors)
        for r in (2, 1, 3):
            x_copy(j, r).start()
            y_copy(j, r).start()

    def second(j):
        for r in (1, 2, 3):
            x_copy(j, r).wait_recv()
        total = sent[j, x, :, :, 0:256].astype(F32)
        for r in range(3):
            total = total + in_x[j, r].astype(F32)
        mid_x[j] = total
        for r in (1, 2, 3):
            y_copy(j, r).wait_recv()
        total = sent[j, :, y, :, 256:512].astype(F32)
        for r in range(3):
            total = total + in_y[j, r].astype(F32)
        mid_y[j] = total
        for r in (2, 1, 3):
            xy_copy(j, r).start()
            yx_copy(j, r).start()

    def third(j):
        for r in (1, 2, 3):
            xy_copy(j, r).wait_recv()
        one = mid_x[j, y]
        for r in range(3):
            one = one + in_xy[j, r]
        for r in (1, 2, 3):
            yx_copy(j, r).wait_recv()
        two = mid_y[j, x]
        for r in range(3):
            two = two + in_yx[j, r]
        for a in range(2):
            last[j, a, :, 0:256] = one[a * 8 : a * 8 + 8]
            last[j, a, :, 256:512] = two[a * 8 : a * 8 + 8]
        for a in range(2):
            @pl.when(z != 2 * j + a)
            def _():
                z_copy(j, a, (z - (2 * j + a) + 8) % 8 - 1).start()

    for j in range(CHUNKS):
        fresh = weigh(j, 0)
        if j:
            acc[...] += cross(BLOCKS - 1, (BLOCKS * j - 1) % 2)
            finish(j - 1)
        weight[(BLOCKS * j) % 2] = fresh
        acc[...] = jnp.zeros_like(acc)

        def one_block(b, carry, j=j):
            slot = (BLOCKS * j + b) % 2
            fresh = weigh(j, b)
            acc[...] += cross(b - 1, 1 - slot)
            weight[slot] = fresh
            return carry

        lax.fori_loop(1, BLOCKS, one_block, 0)
        if j >= 2:
            second(j - 2)
    acc[...] += cross(BLOCKS - 1, (BLOCKS * CHUNKS - 1) % 2)
    finish(CHUNKS - 1)
    third(0)
    second(2)
    third(1)
    second(3)
    third(2)
    third(3)

    for slot in range(7):
        z_copy(0, 0, slot).wait_recv()
    total = last[z // 2, z % 2]
    for slot in range(7):
        total = total + in_z[slot]
    at = pl.multiple_of((x * 4 + y) * 16 + (z % 2) * 8, 8)
    out[...] = own_load[z // 2, pl.ds(at, 8), :] * total / (tails * paths)

    swap.wait_send()

    def drain(r, carry):
        sum_copy(r, (me + r) % 32, me).wait_send()
        stat_copy(r, (me + r) % 32, me).wait_send()
        return carry

    lax.fori_loop(1, 32, drain, 0)
    for j in range(CHUNKS):
        for r in (1, 2, 3):
            x_copy(j, r).wait_send()
            y_copy(j, r).wait_send()
            xy_copy(j, r).wait_send()
            yx_copy(j, r).wait_send()
        for a in range(2):
            @pl.when(z != 2 * j + a)
            def _():
                z_copy(j, a, 0).wait_send()


def body(normals, states, loadings, strikes, hedge, sigma, tail):
    nodes, per_node, factors = normals.shape
    rows = CAP * per_node * 2
    dma = pltpu.SemaphoreType.DMA
    return pl.pallas_call(
        kernel,
        out_shape=jax.ShapeDtypeStruct((8, factors), F32),
        in_specs=[pl.BlockSpec(memory_space=pltpu.HBM)] * 7,
        out_specs=pl.BlockSpec(memory_space=pltpu.VMEM),
        scratch_shapes=[
            pltpu.VMEM(normals.shape, BF16),
            pltpu.VMEM(normals.shape, BF16),
            pltpu.VMEM(loadings.shape, BF16),
            pltpu.VMEM(states.shape, BF16),
            pltpu.VMEM(states.shape, F32),
            pltpu.VMEM((8, 256), F32),
            pltpu.VMEM((8, 256), F32),
            pltpu.VMEM((1, factors), F32),
            pltpu.SMEM(tail.shape, jnp.int32),
            pltpu.SMEM((CAP,), jnp.int32),
            pltpu.SMEM((CAP,), F32),
            pltpu.VMEM((32, 5, 4, 128), F32),
            pltpu.VMEM((32, 5, 4, 128), F32),
            pltpu.VMEM((5, 4, 128), F32),
            pltpu.VMEM((32, 5, 4, 128), F32),
            pltpu.VMEM((CHUNKS, 1, 256), F32),
            pltpu.VMEM((CHUNKS, 1, 256), F32),
            pltpu.VMEM((CHUNKS, 256, factors), F32),
            pltpu.VMEM((CHUNKS, factors, 256), BF16),
            pltpu.VMEM((rows, factors), BF16),
            pltpu.VMEM((128, factors), BF16),
            pltpu.VMEM((BLOCKS, factors, 512), BF16),
            pltpu.VMEM((2, 512, 256), BF16),
            pltpu.VMEM((factors, 256), F32),
            pltpu.VMEM((CHUNKS, 4, 4, 16, factors), BF16),
            pltpu.VMEM((CHUNKS, 3, 4, 16, 256), BF16),
            pltpu.VMEM((CHUNKS, 3, 4, 16, 256), BF16),
            pltpu.VMEM((CHUNKS, 4, 16, 256), F32),
            pltpu.VMEM((CHUNKS, 4, 16, 256), F32),
            pltpu.VMEM((CHUNKS, 3, 16, 256), F32),
            pltpu.VMEM((CHUNKS, 3, 16, 256), F32),
            pltpu.VMEM((CHUNKS, 2, 8, factors), F32),
            pltpu.VMEM((7, 8, factors), F32),
            dma((7,)),
            dma((2,)),
            dma((32,)),
            dma((32,)),
            dma((32,)),
            dma((32,)),
            dma((CHUNKS, 3)),
            dma((CHUNKS, 3)),
            dma((CHUNKS, 3)),
            dma((CHUNKS, 3)),
            dma((CHUNKS, 3)),
            dma((CHUNKS, 3)),
            dma((CHUNKS, 3)),
            dma((CHUNKS, 3)),
            dma((CHUNKS, 2)),
            dma((7,)),
        ],
        compiler_params=pltpu.CompilerParams(
            collective_id=0, has_side_effects=True, vmem_limit_bytes=48 * 1024 * 1024
        ),
    )(
        normals, states, loadings, strikes.reshape(8, 256), hedge.reshape(8, 256),
        sigma.reshape(1, factors), tail,
    )


def solution(mesh):
    in_specs = (P("outer", "inner", None), P("outer", None), P(), P(), P(), P(), P())
    out_specs = P(("outer", "inner"), None)
    return jax.shard_map(body, mesh=mesh, in_specs=in_specs, out_specs=out_specs, check_vma=False)
```

```python
import jax
import jax.numpy as jnp
from jax import lax
from jax.experimental import pallas as pl
from jax.experimental.pallas import tpu as pltpu
from jax.sharding import PartitionSpec as P

CAP = 80
EPSILON = 1e-06
CHUNKS = 4
BLOCKS = 5
MESH = pl.DeviceIdType.MESH
F32 = jnp.float32
BF16 = jnp.bfloat16


def place(hit):
    return jnp.where(hit, 1.0, 0.0)


def offsets():
    span = (0, 1, 2, 1)
    every = [(dx, dy, dc) for dx in range(4) for dy in range(4) for dc in range(2)][1:]
    return sorted(every, key=lambda d: -(span[d[0]] + span[d[1]]))


def code(dx, dy, dc):
    return (dx * 4 + dy) * 2 + dc


def kernel(
    normals, states, loadings, strikes, hedge, sigma, tail, out,
    held, own, pair, load_v, states_b, states_f, strikes_v, hedge_v, sigma_v, tail_s, slot_s, live_s,
    sums, sums_in, stats, half_strike, half_hedge, own_load, load_t,
    mixed, part, turned, weight, sent, in_x, in_y, mid_x, mid_y, in_xy, in_yx, last, in_z,
    copy_sem, pair_sem, sum_out, sum_in, stat_out, stat_in,
    x_out, x_in, y_out, y_in, xy_out, xy_in, yx_out, yx_in, z_out, z_in,
):
    z = lax.axis_index("outer")
    me = lax.axis_index("inner")
    x, y, c = lax.div(me, 8), lax.rem(lax.div(me, 2), 4), lax.rem(me, 2)
    nodes, per_node, factors = held.shape
    paths = per_node * 32
    tails = tail_s.shape[0]
    others = offsets()

    def device(dx, dy, dc):
        return (lax.rem(x + dx, 4) * 4 + lax.rem(y + dy, 4)) * 2 + lax.rem(c + dc, 2)

    copies = [
        (tail, tail_s), (normals, held), (states, states_b), (sigma, sigma_v), (loadings, load_v),
    ]
    for i in range(8):
        copies.append((strikes.at[pl.ds(i * 256, 256)], strikes_v.at[i]))
        copies.append((hedge.at[pl.ds(i * 256, 256)], hedge_v.at[i]))
    loads = [pltpu.make_async_copy(a, b, copy_sem.at[i]) for i, (a, b) in enumerate(copies)]
    loads[0].start()
    loads[1].start()

    barrier = pltpu.get_barrier_semaphore()

    def greet(where):
        pl.semaphore_signal(barrier, inc=1, device_id=where, device_id_type=MESH)

    for d in others:
        greet((z, device(*d)))
    for d in (4, 3, 5, 2, 6, 1, 7):
        greet((lax.rem(z + d, 8), me))
    for item in loads[2:]:
        item.start()

    loads[0].wait()
    first = jnp.int32(0)
    step = tails // 2
    while step:
        first = first + jnp.where(tail_s[first + step - 1] < z * nodes, step, 0)
        step //= 2

    def find(s, carry):
        at = jnp.minimum(first + s, tails - 1)
        node = tail_s[at] - z * nodes
        good = (first + s < tails) & (node >= 0) & (node < nodes)
        slot_s[s] = jnp.clip(node, 0, nodes - 1)
        live_s[s] = jnp.where(good, 1.0, 0.0).astype(F32)
        return carry

    lax.fori_loop(0, CAP, find, 0, unroll=8)
    loads[1].wait()

    def add_up(q, carry):
        for i in range(5):
            rows = held[slot_s[q * 5 + i]]
            own[q * 5 + i] = rows
            block = rows.astype(F32)
            one = jnp.sum(block, axis=0, keepdims=True)
            two = jnp.sum(block * block, axis=0, keepdims=True)
            for h in range(2):
                for b in range(2):
                    lanes = slice(h * 256 + b * 128, h * 256 + b * 128 + 128)
                    sums[q * 2 + h, i, b : b + 1, :] = one[:, lanes]
                    sums[q * 2 + h, i, 2 + b : 3 + b, :] = two[:, lanes]
        return carry

    lax.fori_loop(0, 16, add_up, 0)
    pl.semaphore_wait(barrier, 38)

    def sum_copy(d):
        k = code(*d)
        return pltpu.make_async_remote_copy(
            src_ref=sums.at[device(*d)], dst_ref=sums_in.at[k],
            send_sem=sum_out.at[k], recv_sem=sum_in.at[k],
            device_id=(z, device(*d)), device_id_type=MESH,
        )

    def stat_copy(d):
        k = code(*d)
        return pltpu.make_async_remote_copy(
            src_ref=stats.at[0], dst_ref=stats.at[k],
            send_sem=stat_out.at[k], recv_sem=stat_in.at[k],
            device_id=(z, device(*d)), device_id_type=MESH,
        )

    for d in others:
        sum_copy(d).start()
    swap = pltpu.make_async_remote_copy(
        src_ref=own, dst_ref=pair, send_sem=pair_sem.at[0], recv_sem=pair_sem.at[1],
        device_id=(z, device(0, 0, 1)), device_id_type=MESH,
    )
    swap.start()

    for item in loads[2:]:
        item.wait()
    states_f[...] = states_b[...].astype(F32)
    m_id = lax.broadcasted_iota(jnp.int32, (256, 256), 0)
    l_id = lax.broadcasted_iota(jnp.int32, (256, 256), 1)
    same = (m_id // 16 == l_id // 16) & (m_id % 8 == l_id % 8)
    picks = [same & ((m_id // 8) % 2 == c) & ((l_id // 8) % 2 == a) for a in range(2)]
    picks_t = [same & ((l_id // 8) % 2 == c) & ((m_id // 8) % 2 == a) for a in range(2)]
    for source, target in ((strikes_v, half_strike), (hedge_v, half_hedge)):
        rows = source[...] * 0.5
        moved = [
            jnp.dot(rows, place(pick), precision=lax.Precision.HIGHEST, preferred_element_type=F32)
            for pick in picks
        ]
        for j in range(CHUNKS):
            target[j] = moved[0][2 * j : 2 * j + 1] + moved[1][2 * j + 1 : 2 * j + 2]
    turn = [place(pick).astype(BF16) for pick in picks_t]

    def order(j, carry):
        rows = jnp.zeros((256, factors), F32)
        for a in range(2):
            at = pl.multiple_of((2 * j + a) * 256, 256)
            rows = rows + jnp.dot(turn[a], load_v[pl.ds(at, 256), :], preferred_element_type=F32)
        own_load[j] = rows
        load_t[j] = (rows * 0.5).astype(BF16).T
        return carry

    lax.fori_loop(0, CHUNKS, order, 0)

    total = sums[me]
    for d in reversed(others):
        sum_copy(d).wait_recv()
        total = total + sums_in[code(*d)]
    center = total[:, 0:2, :] / paths
    spread = total[:, 2:4, :] / paths - center * center
    stats[0, :, 0:2, :] = center
    stats[0, :, 2:4, :] = lax.rsqrt(spread + EPSILON)
    for d in others:
        stat_copy(d).start()
    for d in others:
        sum_copy(d).wait_send()
    swap.wait()

    def normalise(g):
        dx = (0, 1, 3, 2)[g]
        for u in range(4):
            dy = (0, 1, 3, 2)[u]
            for dc in range(2):
                if dx or dy or dc:
                    stat_copy((dx, dy, dc)).wait_recv()
        for u in range(4):
            dy = (0, 1, 3, 2)[u]
            q = lax.rem(x + 4 - dx, 4) * 4 + lax.rem(y + 4 - dy, 4)
            for i in range(5):
                s = q * 5 + i
                at, live = slot_s[s], live_s[s]
                state = states_f[pl.ds(at, 1), :]
                for e, source in enumerate((own, pair)):
                    block = source[s]
                    row = (g * 4 + u) * 160 + i * 32 + e * 16
                    for lane in range(4):
                        h, b = lane // 2, lane % 2
                        lanes = slice(lane * 128, lane * 128 + 128)
                        k = code(dx, dy, 0) + lax.rem(c + h, 2)
                        mean = stats[k, i, b : b + 1, :]
                        scale = stats[k, i, 2 + b : 3 + b, :] * live
                        scaled = ((block[:, lanes].astype(F32) - mean) * scale).astype(BF16)
                        both = state[:, lanes] + sigma_v[:, lanes] * scaled.astype(F32)
                        mixed[row : row + 16, lanes] = both.astype(BF16)
                        part[row : row + 16, lanes] = scaled

    def turn_over(g):
        for b in range(5):
            at = g * 640 + b * 128
            turned[:, at : at + 128] = part[at : at + 128, :].T

    def weigh(j, at, count):
        level = jnp.dot(mixed[at : at + count, :], load_t[j], preferred_element_type=F32)
        size = half_hedge[j]
        fresh = size + size * jnp.tanh(level - half_strike[j])
        weight[j % 2, at : at + count, :] = fresh.astype(BF16)

    def x_copy(j, r):
        px = lax.rem(x + r, 4)
        return pltpu.make_async_remote_copy(
            src_ref=sent.at[j, px, :, :, pl.ds(0, 256)], dst_ref=in_x.at[j, r - 1],
            send_sem=x_out.at[j, r - 1], recv_sem=x_in.at[j, r - 1],
            device_id=(z, device(r, 0, 0)), device_id_type=MESH,
        )

    def y_copy(j, r):
        py = lax.rem(y + r, 4)
        return pltpu.make_async_remote_copy(
            src_ref=sent.at[j, :, py, :, pl.ds(256, 256)], dst_ref=in_y.at[j, r - 1],
            send_sem=y_out.at[j, r - 1], recv_sem=y_in.at[j, r - 1],
            device_id=(z, device(0, r, 0)), device_id_type=MESH,
        )

    def xy_copy(j, r):
        py = lax.rem(y + r, 4)
        return pltpu.make_async_remote_copy(
            src_ref=mid_x.at[j, py], dst_ref=in_xy.at[j, r - 1],
            send_sem=xy_out.at[j, r - 1], recv_sem=xy_in.at[j, r - 1],
            device_id=(z, device(0, r, 0)), device_id_type=MESH,
        )

    def yx_copy(j, r):
        px = lax.rem(x + r, 4)
        return pltpu.make_async_remote_copy(
            src_ref=mid_y.at[j, px], dst_ref=in_yx.at[j, r - 1],
            send_sem=yx_out.at[j, r - 1], recv_sem=yx_in.at[j, r - 1],
            device_id=(z, device(r, 0, 0)), device_id_type=MESH,
        )

    def z_copy(j, a, slot):
        return pltpu.make_async_remote_copy(
            src_ref=last.at[j, a], dst_ref=in_z.at[slot],
            send_sem=z_out.at[j, a], recv_sem=z_in.at[slot],
            device_id=(2 * j + a, me), device_id_type=MESH,
        )

    def finish(j):
        rows = jnp.dot(turned[...], weight[j % 2], preferred_element_type=F32)
        sent[j] = rows.astype(BF16).T.reshape(4, 4, 16, factors)
        for r in (2, 1, 3):
            x_copy(j, r).start()
            y_copy(j, r).start()

    def second(j):
        for r in (1, 3, 2):
            x_copy(j, r).wait_recv()
        total = sent[j, x, :, :, 0:256].astype(F32)
        for r in range(3):
            total = total + in_x[j, r].astype(F32)
        mid_x[j] = total
        for r in (1, 3, 2):
            y_copy(j, r).wait_recv()
        for r in (2, 1, 3):
            xy_copy(j, r).start()
        total = sent[j, :, y, :, 256:512].astype(F32)
        for r in range(3):
            total = total + in_y[j, r].astype(F32)
        mid_y[j] = total
        for r in (2, 1, 3):
            yx_copy(j, r).start()

    def third(j):
        for r in (1, 3, 2):
            xy_copy(j, r).wait_recv()
        one = mid_x[j, y]
        for r in range(3):
            one = one + in_xy[j, r]
        for r in (1, 3, 2):
            yx_copy(j, r).wait_recv()
        two = mid_y[j, x]
        for r in range(3):
            two = two + in_yx[j, r]
        for a in range(2):
            last[j, a, :, 0:256] = one[a * 8 : a * 8 + 8]
            last[j, a, :, 256:512] = two[a * 8 : a * 8 + 8]
        for a in range(2):
            @pl.when(z != 2 * j + a)
            def _():
                z_copy(j, a, lax.rem(z - (2 * j + a) + 8, 8) - 1).start()

    for g in range(4):
        normalise(g)
        if g:
            turn_over(g - 1)
            weigh(0, (g - 1) * 640, 640)
    turn_over(3)
    weigh(0, 1920, 640)
    for j in range(1, CHUNKS + 1):
        if j < CHUNKS:
            for b in range(BLOCKS):
                weigh(j, b * 512, 512)
        finish(j - 1)
    for d in others:
        stat_copy(d).wait_send()
    for j in range(CHUNKS):
        second(j)
    for j in range(CHUNKS):
        for r in (1, 2, 3):
            x_copy(j, r).wait_send()
            y_copy(j, r).wait_send()
    for j in range(CHUNKS):
        third(j)

    for j in range(CHUNKS):
        for r in (1, 2, 3):
            xy_copy(j, r).wait_send()
            yx_copy(j, r).wait_send()
    for slot in range(7):
        z_copy(0, 0, slot).wait_recv()
    total = last[lax.div(z, 2), lax.rem(z, 2)]
    for slot in range(7):
        total = total + in_z[slot]
    at = pl.multiple_of((x * 4 + y) * 16 + lax.rem(z, 2) * 8, 8)
    out[...] = own_load[lax.div(z, 2), pl.ds(at, 8), :] * total / (tails * paths)

    for j in range(CHUNKS):
        for a in range(2):
            @pl.when(z != 2 * j + a)
            def _():
                z_copy(j, a, 0).wait_send()


def body(normals, states, loadings, strikes, hedge, sigma, tail):
    nodes, per_node, factors = normals.shape
    rows = CAP * per_node * 2
    dma = pltpu.SemaphoreType.DMA
    return pl.pallas_call(
        kernel,
        out_shape=jax.ShapeDtypeStruct((8, factors), F32),
        in_specs=[pl.BlockSpec(memory_space=pltpu.HBM)] * 7,
        out_specs=pl.BlockSpec(memory_space=pltpu.VMEM),
        scratch_shapes=[
            pltpu.VMEM(normals.shape, BF16),
            pltpu.VMEM((CAP, per_node, factors), BF16),
            pltpu.VMEM((CAP, per_node, factors), BF16),
            pltpu.VMEM(loadings.shape, BF16),
            pltpu.VMEM(states.shape, BF16),
            pltpu.VMEM(states.shape, F32),
            pltpu.VMEM((8, 256), F32),
            pltpu.VMEM((8, 256), F32),
            pltpu.VMEM((1, factors), F32),
            pltpu.SMEM(tail.shape, jnp.int32),
            pltpu.SMEM((CAP,), jnp.int32),
            pltpu.SMEM((CAP,), F32),
            pltpu.VMEM((32, 5, 4, 128), F32),
            pltpu.VMEM((32, 5, 4, 128), F32),
            pltpu.VMEM((32, 5, 4, 128), F32),
            pltpu.VMEM((CHUNKS, 1, 256), F32),
            pltpu.VMEM((CHUNKS, 1, 256), F32),
            pltpu.VMEM((CHUNKS, 256, factors), F32),
            pltpu.VMEM((CHUNKS, factors, 256), BF16),
            pltpu.VMEM((rows, factors), BF16),
            pltpu.VMEM((rows, factors), BF16),
            pltpu.VMEM((factors, rows), BF16),
            pltpu.VMEM((2, rows, 256), BF16),
            pltpu.VMEM((CHUNKS, 4, 4, 16, factors), BF16),
            pltpu.VMEM((CHUNKS, 3, 4, 16, 256), BF16),
            pltpu.VMEM((CHUNKS, 3, 4, 16, 256), BF16),
            pltpu.VMEM((CHUNKS, 4, 16, 256), F32),
            pltpu.VMEM((CHUNKS, 4, 16, 256), F32),
            pltpu.VMEM((CHUNKS, 3, 16, 256), F32),
            pltpu.VMEM((CHUNKS, 3, 16, 256), F32),
            pltpu.VMEM((CHUNKS, 2, 8, factors), F32),
            pltpu.VMEM((7, 8, factors), F32),
            dma((21,)),
            dma((2,)),
            dma((32,)),
            dma((32,)),
            dma((32,)),
            dma((32,)),
            dma((CHUNKS, 3)),
            dma((CHUNKS, 3)),
            dma((CHUNKS, 3)),
            dma((CHUNKS, 3)),
            dma((CHUNKS, 3)),
            dma((CHUNKS, 3)),
            dma((CHUNKS, 3)),
            dma((CHUNKS, 3)),
            dma((CHUNKS, 2)),
            dma((7,)),
        ],
        compiler_params=pltpu.CompilerParams(
            collective_id=0, has_side_effects=True, vmem_limit_bytes=63 * 1024 * 1024
        ),
    )(
        normals, states, loadings, strikes, hedge, sigma.reshape(1, factors), tail,
    )


def solution(mesh):
    in_specs = (P("outer", "inner", None), P("outer", None), P(), P(), P(), P(), P())
    out_specs = P(("outer", "inner"), None)
    return jax.shard_map(body, mesh=mesh, in_specs=in_specs, out_specs=out_specs, check_vma=False)
```

```python
import jax
import jax.numpy as jnp
from jax import lax
from jax.experimental import pallas as pl
from jax.experimental.pallas import tpu as pltpu
from jax.sharding import PartitionSpec as P

CAP = 80
EPSILON = 1e-06
CHUNKS = 4
BLOCKS = 5
MESH = pl.DeviceIdType.MESH
F32 = jnp.float32
BF16 = jnp.bfloat16


def place(hit):
    return jnp.where(hit, 1.0, 0.0)


def offsets():
    span = (0, 1, 2, 1)
    every = [(dx, dy) for dx in range(4) for dy in range(4)][1:]
    return sorted(every, key=lambda d: -(span[d[0]] + span[d[1]]))


def kernel(
    normals, states, loadings, strikes, hedge, sigma, tail, out,
    held, own, pair, load_v, states_b, states_f, strikes_v, hedge_v, sigma_v, sigma_f, tail_s, slot_s, live_s,
    sums, sums_pair, sums_chip, sums_in, stats, half_strike, half_hedge, own_load, load_t,
    mixed, part, turned, weight, sent, in_x, in_y, mid_x, mid_y, in_xy, in_yx, last, in_z,
    copy_sem, pair_sem, join_sem, pass_sem, sum_out, sum_in, stat_out, stat_in,
    x_out, x_in, y_out, y_in, xy_out, xy_in, yx_out, yx_in, z_out, z_in,
):
    z = lax.axis_index("outer")
    me = lax.axis_index("inner")
    x, y, c = lax.div(me, 8), lax.rem(lax.div(me, 2), 4), lax.rem(me, 2)
    nodes, per_node, factors = held.shape
    paths = per_node * 32
    tails = tail_s.shape[0]
    others = offsets()

    def device(dx, dy, dc):
        return (lax.rem(x + dx, 4) * 4 + lax.rem(y + dy, 4)) * 2 + lax.rem(c + dc, 2)

    copies = [
        (tail, tail_s), (normals, held), (states, states_b), (sigma, sigma_v), (loadings, load_v),
    ]
    for i in range(8):
        copies.append((strikes.at[pl.ds(i * 256, 256)], strikes_v.at[i]))
        copies.append((hedge.at[pl.ds(i * 256, 256)], hedge_v.at[i]))
    loads = [pltpu.make_async_copy(a, b, copy_sem.at[i]) for i, (a, b) in enumerate(copies)]
    loads[0].start()
    loads[1].start()

    barrier = pltpu.get_barrier_semaphore()

    def greet(where):
        pl.semaphore_signal(barrier, inc=1, device_id=where, device_id_type=MESH)

    for dx, dy in others:
        greet((z, device(dx, dy, 0)))
    for d in (4, 3, 5, 2, 6, 1, 7):
        greet((lax.rem(z + d, 8), me))
    partner = (z, device(0, 0, 1))
    greet(partner)
    for item in loads[2:]:
        item.start()

    loads[0].wait()
    first = jnp.int32(0)
    step = tails // 2
    while step:
        first = first + jnp.where(tail_s[first + step - 1] < z * nodes, step, 0)
        step //= 2

    def find(s, carry):
        at = jnp.minimum(first + s, tails - 1)
        node = tail_s[at] - z * nodes
        good = (first + s < tails) & (node >= 0) & (node < nodes)
        slot_s[s] = jnp.clip(node, 0, nodes - 1)
        live_s[s] = jnp.where(good, 1.0, 0.0).astype(F32)
        return carry

    lax.fori_loop(0, CAP, find, 0, unroll=8)
    loads[1].wait()

    def add_up(q, carry):
        for i in range(5):
            rows = held[slot_s[q * 5 + i]]
            own[q * 5 + i] = rows
            block = rows.astype(F32)
            one = jnp.sum(block, axis=0, keepdims=True)
            two = jnp.sum(block * block, axis=0, keepdims=True)
            for h in range(2):
                for b in range(2):
                    lanes = slice(h * 256 + b * 128, h * 256 + b * 128 + 128)
                    sums[h, q, i, b : b + 1, :] = one[:, lanes]
                    sums[h, q, i, 2 + b : 3 + b, :] = two[:, lanes]
        return carry

    lax.fori_loop(0, 16, add_up, 0)
    pl.semaphore_wait(barrier, 23)

    join = pltpu.make_async_remote_copy(
        src_ref=sums.at[1 - c], dst_ref=sums_pair, send_sem=join_sem.at[0], recv_sem=join_sem.at[1],
        device_id=partner, device_id_type=MESH,
    )
    join.start()
    for item in loads[2:]:
        item.wait()
    for b in range(4):
        lanes = slice(b * 128, b * 128 + 128)
        states_f[b] = states_b[:, lanes].astype(F32)
        sigma_f[b] = sigma_v[:, lanes]
    join.wait_recv()
    sums_chip[...] = sums[c] + sums_pair[...]

    def sum_copy(d):
        dx, dy = d
        return pltpu.make_async_remote_copy(
            src_ref=sums_chip.at[lax.rem(x + dx, 4) * 4 + lax.rem(y + dy, 4)],
            dst_ref=sums_in.at[dx * 4 + dy],
            send_sem=sum_out.at[dx * 4 + dy], recv_sem=sum_in.at[dx * 4 + dy],
            device_id=(z, device(dx, dy, 0)), device_id_type=MESH,
        )

    def stat_copy(d):
        dx, dy = d
        return pltpu.make_async_remote_copy(
            src_ref=stats.at[0, 0], dst_ref=stats.at[0, dx * 4 + dy],
            send_sem=stat_out.at[dx * 4 + dy], recv_sem=stat_in.at[dx * 4 + dy],
            device_id=(z, device(dx, dy, 0)), device_id_type=MESH,
        )

    for d in others:
        sum_copy(d).start()
    swap = pltpu.make_async_remote_copy(
        src_ref=own, dst_ref=pair, send_sem=pair_sem.at[0], recv_sem=pair_sem.at[1],
        device_id=partner, device_id_type=MESH,
    )
    swap.start()

    m_id = lax.broadcasted_iota(jnp.int32, (256, 256), 0)
    l_id = lax.broadcasted_iota(jnp.int32, (256, 256), 1)
    same = (m_id // 16 == l_id // 16) & (m_id % 8 == l_id % 8)
    picks = [same & ((m_id // 8) % 2 == c) & ((l_id // 8) % 2 == a) for a in range(2)]
    picks_t = [same & ((l_id // 8) % 2 == c) & ((m_id // 8) % 2 == a) for a in range(2)]
    for source, target in ((strikes_v, half_strike), (hedge_v, half_hedge)):
        rows = source[...] * 0.5
        moved = [
            jnp.dot(rows, place(pick), precision=lax.Precision.HIGHEST, preferred_element_type=F32)
            for pick in picks
        ]
        for j in range(CHUNKS):
            target[j] = moved[0][2 * j : 2 * j + 1] + moved[1][2 * j + 1 : 2 * j + 2]
    turn = [place(pick).astype(BF16) for pick in picks_t]

    def order(j, carry):
        rows = jnp.zeros((256, factors), F32)
        for a in range(2):
            at = pl.multiple_of((2 * j + a) * 256, 256)
            rows = rows + jnp.dot(turn[a], load_v[pl.ds(at, 256), :], preferred_element_type=F32)
        own_load[j] = rows
        load_t[j] = (rows * 0.5).astype(BF16).T
        return carry

    lax.fori_loop(0, CHUNKS, order, 0)

    total = sums_chip[x * 4 + y]
    for d in reversed(others):
        sum_copy(d).wait_recv()
        total = total + sums_in[d[0] * 4 + d[1]]
    center = total[:, 0:2, :] / paths
    spread = total[:, 2:4, :] / paths - center * center
    stats[0, 0, :, 0:2, :] = center
    stats[0, 0, :, 2:4, :] = lax.rsqrt(spread + EPSILON)
    for d in others:
        stat_copy(d).start()
    for d in others:
        sum_copy(d).wait_send()
    join.wait_send()
    swap.wait()
    for d in reversed(others):
        stat_copy(d).wait_recv()
    give = pltpu.make_async_remote_copy(
        src_ref=stats.at[0], dst_ref=stats.at[1], send_sem=pass_sem.at[0], recv_sem=pass_sem.at[1],
        device_id=partner, device_id_type=MESH,
    )
    give.start()

    def normalise(g, e):
        base = (c if e == 0 else 1 - c) * 2
        for dy in range(4):
            q = lax.rem(x + 4 - g, 4) * 4 + lax.rem(y + 4 - dy, 4)
            for i in range(5):
                s = q * 5 + i
                at, live = slot_s[s], live_s[s]
                for b in range(2):
                    lanes = pl.ds(pl.multiple_of((base + b) * 128, 128), 128)
                    state = states_f[base + b, pl.ds(at, 1), :]
                    mean = stats[e, g * 4 + dy, i, b : b + 1, :]
                    scale = stats[e, g * 4 + dy, i, 2 + b : 3 + b, :] * live
                    for w, source in enumerate((own, pair)):
                        row = (g * 4 + dy) * 160 + i * 32 + w * 16
                        block = source[s, :, lanes].astype(F32)
                        scaled = ((block - mean) * scale).astype(BF16)
                        both = state + sigma_f[base + b] * scaled.astype(F32)
                        mixed[row : row + 16, lanes] = both.astype(BF16)
                        part[row : row + 16, lanes] = scaled

    def turn_over(g):
        for b in range(5):
            at = g * 640 + b * 128
            turned[:, at : at + 128] = part[at : at + 128, :].T

    def weigh(j, at, count):
        level = jnp.dot(mixed[at : at + count, :], load_t[j], preferred_element_type=F32)
        size = half_hedge[j]
        fresh = size + size * jnp.tanh(level - half_strike[j])
        weight[j % 2, at : at + count, :] = fresh.astype(BF16)

    def x_copy(j, r):
        px = lax.rem(x + r, 4)
        return pltpu.make_async_remote_copy(
            src_ref=sent.at[j, px, :, :, pl.ds(0, 256)], dst_ref=in_x.at[j, r - 1],
            send_sem=x_out.at[j, r - 1], recv_sem=x_in.at[j, r - 1],
            device_id=(z, device(r, 0, 0)), device_id_type=MESH,
        )

    def y_copy(j, r):
        py = lax.rem(y + r, 4)
        return pltpu.make_async_remote_copy(
            src_ref=sent.at[j, :, py, :, pl.ds(256, 256)], dst_ref=in_y.at[j, r - 1],
            send_sem=y_out.at[j, r - 1], recv_sem=y_in.at[j, r - 1],
            device_id=(z, device(0, r, 0)), device_id_type=MESH,
        )

    def xy_copy(j, r):
        py = lax.rem(y + r, 4)
        return pltpu.make_async_remote_copy(
            src_ref=mid_x.at[j, py], dst_ref=in_xy.at[j, r - 1],
            send_sem=xy_out.at[j, r - 1], recv_sem=xy_in.at[j, r - 1],
            device_id=(z, device(0, r, 0)), device_id_type=MESH,
        )

    def yx_copy(j, r):
        px = lax.rem(x + r, 4)
        return pltpu.make_async_remote_copy(
            src_ref=mid_y.at[j, px], dst_ref=in_yx.at[j, r - 1],
            send_sem=yx_out.at[j, r - 1], recv_sem=yx_in.at[j, r - 1],
            device_id=(z, device(r, 0, 0)), device_id_type=MESH,
        )

    def z_copy(j, a, slot):
        return pltpu.make_async_remote_copy(
            src_ref=last.at[j, a], dst_ref=in_z.at[slot],
            send_sem=z_out.at[j, a], recv_sem=z_in.at[slot],
            device_id=(2 * j + a, me), device_id_type=MESH,
        )

    def finish(j):
        rows = jnp.dot(turned[...], weight[j % 2], preferred_element_type=F32)
        sent[j] = rows.astype(BF16).T.reshape(4, 4, 16, factors)
        for r in (2, 1, 3):
            x_copy(j, r).start()
            y_copy(j, r).start()

    def second(j):
        for r in (1, 3, 2):
            x_copy(j, r).wait_recv()
        total = sent[j, x, :, :, 0:256].astype(F32)
        for r in range(3):
            total = total + in_x[j, r].astype(F32)
        mid_x[j] = total
        for r in (1, 3, 2):
            y_copy(j, r).wait_recv()
        for r in (2, 1, 3):
            xy_copy(j, r).start()
        total = sent[j, :, y, :, 256:512].astype(F32)
        for r in range(3):
            total = total + in_y[j, r].astype(F32)
        mid_y[j] = total
        for r in (2, 1, 3):
            yx_copy(j, r).start()

    def third(j):
        for r in (1, 3, 2):
            xy_copy(j, r).wait_recv()
        one = mid_x[j, y]
        for r in range(3):
            one = one + in_xy[j, r]
        for r in (1, 3, 2):
            yx_copy(j, r).wait_recv()
        two = mid_y[j, x]
        for r in range(3):
            two = two + in_yx[j, r]
        for a in range(2):
            last[j, a, :, 0:256] = one[a * 8 : a * 8 + 8]
            last[j, a, :, 256:512] = two[a * 8 : a * 8 + 8]
        for a in range(2):
            @pl.when(z != 2 * j + a)
            def _():
                z_copy(j, a, lax.rem(z - (2 * j + a) + 8, 8) - 1).start()

    for g in range(4):
        normalise(g, 0)
    give.wait_recv()
    for g in range(4):
        normalise(g, 1)
        if g:
            turn_over(g - 1)
            weigh(0, (g - 1) * 640, 640)
    turn_over(3)
    weigh(0, 1920, 640)
    for j in range(1, CHUNKS + 1):
        if j < CHUNKS:
            for b in range(BLOCKS):
                weigh(j, b * 512, 512)
        finish(j - 1)
    give.wait_send()
    for d in others:
        stat_copy(d).wait_send()
    second(0)
    second(1)
    second(2)
    third(0)
    for j in range(CHUNKS):
        for r in (1, 2, 3):
            x_copy(j, r).wait_send()
            y_copy(j, r).wait_send()
    second(3)
    third(1)
    third(2)
    third(3)

    for j in range(CHUNKS):
        for r in (1, 2, 3):
            xy_copy(j, r).wait_send()
            yx_copy(j, r).wait_send()
    for slot in range(7):
        z_copy(0, 0, slot).wait_recv()
    total = last[lax.div(z, 2), lax.rem(z, 2)]
    for slot in range(7):
        total = total + in_z[slot]
    at = pl.multiple_of((x * 4 + y) * 16 + lax.rem(z, 2) * 8, 8)
    out[...] = own_load[lax.div(z, 2), pl.ds(at, 8), :] * total / (tails * paths)

    for j in range(CHUNKS):
        for a in range(2):
            @pl.when(z != 2 * j + a)
            def _():
                z_copy(j, a, 0).wait_send()


def body(normals, states, loadings, strikes, hedge, sigma, tail):
    nodes, per_node, factors = normals.shape
    rows = CAP * per_node * 2
    dma = pltpu.SemaphoreType.DMA
    return pl.pallas_call(
        kernel,
        out_shape=jax.ShapeDtypeStruct((8, factors), F32),
        in_specs=[pl.BlockSpec(memory_space=pltpu.HBM)] * 7,
        out_specs=pl.BlockSpec(memory_space=pltpu.VMEM),
        scratch_shapes=[
            pltpu.VMEM(normals.shape, BF16),
            pltpu.VMEM((CAP, per_node, factors), BF16),
            pltpu.VMEM((CAP, per_node, factors), BF16),
            pltpu.VMEM(loadings.shape, BF16),
            pltpu.VMEM(states.shape, BF16),
            pltpu.VMEM((4, nodes, 128), F32),
            pltpu.VMEM((8, 256), F32),
            pltpu.VMEM((8, 256), F32),
            pltpu.VMEM((1, factors), F32),
            pltpu.VMEM((4, 1, 128), F32),
            pltpu.SMEM(tail.shape, jnp.int32),
            pltpu.SMEM((CAP,), jnp.int32),
            pltpu.SMEM((CAP,), F32),
            pltpu.VMEM((2, 16, 5, 4, 128), F32),
            pltpu.VMEM((16, 5, 4, 128), F32),
            pltpu.VMEM((16, 5, 4, 128), F32),
            pltpu.VMEM((16, 5, 4, 128), F32),
            pltpu.VMEM((2, 16, 5, 4, 128), F32),
            pltpu.VMEM((CHUNKS, 1, 256), F32),
            pltpu.VMEM((CHUNKS, 1, 256), F32),
            pltpu.VMEM((CHUNKS, 256, factors), F32),
            pltpu.VMEM((CHUNKS, factors, 256), BF16),
            pltpu.VMEM((rows, factors), BF16),
            pltpu.VMEM((rows, factors), BF16),
            pltpu.VMEM((factors, rows), BF16),
            pltpu.VMEM((2, rows, 256), BF16),
            pltpu.VMEM((CHUNKS, 4, 4, 16, factors), BF16),
            pltpu.VMEM((CHUNKS, 3, 4, 16, 256), BF16),
            pltpu.VMEM((CHUNKS, 3, 4, 16, 256), BF16),
            pltpu.VMEM((CHUNKS, 4, 16, 256), F32),
            pltpu.VMEM((CHUNKS, 4, 16, 256), F32),
            pltpu.VMEM((CHUNKS, 3, 16, 256), F32),
            pltpu.VMEM((CHUNKS, 3, 16, 256), F32),
            pltpu.VMEM((CHUNKS, 2, 8, factors), F32),
            pltpu.VMEM((7, 8, factors), F32),
            dma((21,)),
            dma((2,)),
            dma((2,)),
            dma((2,)),
            dma((16,)),
            dma((16,)),
            dma((16,)),
            dma((16,)),
            dma((CHUNKS, 3)),
            dma((CHUNKS, 3)),
            dma((CHUNKS, 3)),
            dma((CHUNKS, 3)),
            dma((CHUNKS, 3)),
            dma((CHUNKS, 3)),
            dma((CHUNKS, 3)),
            dma((CHUNKS, 3)),
            dma((CHUNKS, 2)),
            dma((7,)),
        ],
        compiler_params=pltpu.CompilerParams(
            collective_id=0, has_side_effects=True, vmem_limit_bytes=63 * 1024 * 1024
        ),
    )(
        normals, states, loadings, strikes, hedge, sigma.reshape(1, factors), tail,
    )


def solution(mesh):
    in_specs = (P("outer", "inner", None), P("outer", None), P(), P(), P(), P(), P())
    out_specs = P(("outer", "inner"), None)
    return jax.shard_map(body, mesh=mesh, in_specs=in_specs, out_specs=out_specs, check_vma=False)
```

```python
import jax
import jax.numpy as jnp
from jax import lax
from jax.experimental import pallas as pl
from jax.experimental.pallas import tpu as pltpu
from jax.sharding import PartitionSpec as P

CAP = 80
EPSILON = 1e-06
CHUNKS = 4
MESH = pl.DeviceIdType.MESH
F32 = jnp.float32
BF16 = jnp.bfloat16


def place(hit):
    return jnp.where(hit, 1.0, 0.0)


def offsets():
    span = (0, 1, 2, 1)
    every = [(dx, dy) for dx in range(4) for dy in range(4)][1:]
    return sorted(every, key=lambda d: -(span[d[0]] + span[d[1]]))


def kernel(
    normals, states, loadings, strikes, hedge, sigma, tail, out,
    held, own, pair, load_v, states_b, states_f, strikes_v, hedge_v, sigma_v, sigma_f, tail_s, slot_s, live_s,
    sums, sums_pair, sums_chip, sums_in, stats, half_strike, half_hedge, own_load, load_t,
    mixed, part, turned, weight, sent, in_x, in_y, mid_x, mid_y, in_xy, in_yx, last, in_z,
    copy_sem, pair_sem, join_sem, pass_sem, sum_out, sum_in, stat_out, stat_in,
    x_out, x_in, y_out, y_in, xy_out, xy_in, yx_out, yx_in, z_out, z_in,
):
    z = lax.axis_index("outer")
    me = lax.axis_index("inner")
    x, y, c = lax.div(me, 8), lax.rem(lax.div(me, 2), 4), lax.rem(me, 2)
    nodes, per_node, factors = held.shape
    paths = per_node * 32
    tails = tail_s.shape[0]
    others = offsets()

    def device(dx, dy, dc):
        return (lax.rem(x + dx, 4) * 4 + lax.rem(y + dy, 4)) * 2 + lax.rem(c + dc, 2)

    copies = [
        (tail, tail_s), (normals, held), (states, states_b), (sigma, sigma_v), (loadings, load_v),
    ]
    for i in range(8):
        copies.append((strikes.at[pl.ds(i * 256, 256)], strikes_v.at[i]))
        copies.append((hedge.at[pl.ds(i * 256, 256)], hedge_v.at[i]))
    loads = [pltpu.make_async_copy(a, b, copy_sem.at[i]) for i, (a, b) in enumerate(copies)]
    loads[0].start()
    loads[1].start()

    barrier = pltpu.get_barrier_semaphore()

    def greet(where):
        pl.semaphore_signal(barrier, inc=1, device_id=where, device_id_type=MESH)

    for dx, dy in others:
        greet((z, device(dx, dy, 0)))
    for d in (4, 3, 5, 2, 6, 1, 7):
        greet((lax.rem(z + d, 8), me))
    partner = (z, device(0, 0, 1))
    greet(partner)
    for item in loads[2:]:
        item.start()

    loads[0].wait()
    first = jnp.int32(0)
    step = tails // 2
    while step:
        first = first + jnp.where(tail_s[first + step - 1] < z * nodes, step, 0)
        step //= 2

    def find(s, carry):
        at = jnp.minimum(first + s, tails - 1)
        node = tail_s[at] - z * nodes
        good = (first + s < tails) & (node >= 0) & (node < nodes)
        slot_s[s] = jnp.clip(node, 0, nodes - 1)
        live_s[s] = jnp.where(good, 1.0, 0.0).astype(F32)
        return carry

    lax.fori_loop(0, CAP, find, 0, unroll=8)
    loads[1].wait()

    def add_up(q, carry):
        for i in range(5):
            rows = held[slot_s[q * 5 + i]]
            own[q * 5 + i] = rows
            block = rows.astype(F32)
            one = jnp.sum(block, axis=0, keepdims=True)
            two = jnp.sum(block * block, axis=0, keepdims=True)
            for h in range(2):
                for b in range(2):
                    lanes = slice(h * 256 + b * 128, h * 256 + b * 128 + 128)
                    sums[h, q, i, b : b + 1, :] = one[:, lanes]
                    sums[h, q, i, 2 + b : 3 + b, :] = two[:, lanes]
        return carry

    lax.fori_loop(0, 16, add_up, 0)
    pl.semaphore_wait(barrier, 23)

    join = pltpu.make_async_remote_copy(
        src_ref=sums.at[1 - c], dst_ref=sums_pair, send_sem=join_sem.at[0], recv_sem=join_sem.at[1],
        device_id=partner, device_id_type=MESH,
    )
    join.start()
    for item in loads[2:]:
        item.wait()
    for b in range(4):
        lanes = slice(b * 128, b * 128 + 128)
        states_f[b] = states_b[:, lanes].astype(F32)
        sigma_f[b] = sigma_v[:, lanes]
    join.wait_recv()
    sums_chip[...] = sums[c] + sums_pair[...]

    def sum_copy(d):
        dx, dy = d
        return pltpu.make_async_remote_copy(
            src_ref=sums_chip.at[lax.rem(x + dx, 4) * 4 + lax.rem(y + dy, 4)],
            dst_ref=sums_in.at[dx * 4 + dy],
            send_sem=sum_out.at[dx * 4 + dy], recv_sem=sum_in.at[dx * 4 + dy],
            device_id=(z, device(dx, dy, 0)), device_id_type=MESH,
        )

    def stat_copy(d):
        dx, dy = d
        return pltpu.make_async_remote_copy(
            src_ref=stats.at[0, 0], dst_ref=stats.at[0, dx * 4 + dy],
            send_sem=stat_out.at[dx * 4 + dy], recv_sem=stat_in.at[dx * 4 + dy],
            device_id=(z, device(dx, dy, 0)), device_id_type=MESH,
        )

    for d in others:
        sum_copy(d).start()
    swap = pltpu.make_async_remote_copy(
        src_ref=own, dst_ref=pair, send_sem=pair_sem.at[0], recv_sem=pair_sem.at[1],
        device_id=partner, device_id_type=MESH,
    )
    swap.start()

    m_id = lax.broadcasted_iota(jnp.int32, (256, 256), 0)
    l_id = lax.broadcasted_iota(jnp.int32, (256, 256), 1)
    same = (m_id // 16 == l_id // 16) & (m_id % 8 == l_id % 8)
    picks = [same & ((m_id // 8) % 2 == c) & ((l_id // 8) % 2 == a) for a in range(2)]
    picks_t = [same & ((l_id // 8) % 2 == c) & ((m_id // 8) % 2 == a) for a in range(2)]
    for source, target in ((strikes_v, half_strike), (hedge_v, half_hedge)):
        rows = source[...] * 0.5
        moved = [
            jnp.dot(rows, place(pick), precision=lax.Precision.HIGHEST, preferred_element_type=F32)
            for pick in picks
        ]
        for j in range(CHUNKS):
            target[j] = moved[0][2 * j : 2 * j + 1] + moved[1][2 * j + 1 : 2 * j + 2]
    turn = [place(pick).astype(BF16) for pick in picks_t]

    def order(j, carry):
        rows = jnp.zeros((256, factors), F32)
        for a in range(2):
            at = pl.multiple_of((2 * j + a) * 256, 256)
            rows = rows + jnp.dot(turn[a], load_v[pl.ds(at, 256), :], preferred_element_type=F32)
        own_load[j] = rows
        load_t[j] = (rows * 0.5).astype(BF16).T
        return carry

    lax.fori_loop(0, CHUNKS, order, 0)

    total = sums_chip[x * 4 + y]
    for d in reversed(others):
        sum_copy(d).wait_recv()
        total = total + sums_in[d[0] * 4 + d[1]]
    center = total[:, 0:2, :] / paths
    spread = total[:, 2:4, :] / paths - center * center
    stats[0, 0, :, 0:2, :] = center
    stats[0, 0, :, 2:4, :] = lax.rsqrt(spread + EPSILON)
    for d in others:
        stat_copy(d).start()
    for d in others:
        sum_copy(d).wait_send()
    join.wait_send()
    swap.wait()
    for d in reversed(others):
        stat_copy(d).wait_recv()
    give = pltpu.make_async_remote_copy(
        src_ref=stats.at[0], dst_ref=stats.at[1], send_sem=pass_sem.at[0], recv_sem=pass_sem.at[1],
        device_id=partner, device_id_type=MESH,
    )
    give.start()

    def normalise(g, e):
        base = (c if e == 0 else 1 - c) * 2
        for dy in range(4):
            q = lax.rem(x + 4 - g, 4) * 4 + lax.rem(y + 4 - dy, 4)
            for i in range(5):
                s = q * 5 + i
                at, live = slot_s[s], live_s[s]
                for b in range(2):
                    lanes = pl.ds(pl.multiple_of((base + b) * 128, 128), 128)
                    state = states_f[base + b, pl.ds(at, 1), :]
                    mean = stats[e, g * 4 + dy, i, b : b + 1, :]
                    scale = stats[e, g * 4 + dy, i, 2 + b : 3 + b, :] * live
                    for w, source in enumerate((own, pair)):
                        row = (g * 4 + dy) * 160 + i * 32 + w * 16
                        block = source[s, :, lanes].astype(F32)
                        scaled = ((block - mean) * scale).astype(BF16)
                        both = state + sigma_f[base + b] * scaled.astype(F32)
                        mixed[row : row + 16, lanes] = both.astype(BF16)
                        part[row : row + 16, lanes] = scaled

    def turn_over(g):
        for b in range(5):
            at = g * 640 + b * 128
            turned[:, at : at + 128] = part[at : at + 128, :].T

    def weigh(j, at, count):
        level = jnp.dot(mixed[at : at + count, :], load_t[j], preferred_element_type=F32)
        size = half_hedge[j]
        fresh = size + size * jnp.tanh(level - half_strike[j])
        weight[j % 2, at : at + count, :] = fresh.astype(BF16)

    def x_copy(j, r):
        px = lax.rem(x + r, 4)
        return pltpu.make_async_remote_copy(
            src_ref=sent.at[j, px, :, :, pl.ds(0, 256)], dst_ref=in_x.at[j, r - 1],
            send_sem=x_out.at[j, r - 1], recv_sem=x_in.at[j, r - 1],
            device_id=(z, device(r, 0, 0)), device_id_type=MESH,
        )

    def y_copy(j, r):
        py = lax.rem(y + r, 4)
        return pltpu.make_async_remote_copy(
            src_ref=sent.at[j, :, py, :, pl.ds(256, 256)], dst_ref=in_y.at[j, r - 1],
            send_sem=y_out.at[j, r - 1], recv_sem=y_in.at[j, r - 1],
            device_id=(z, device(0, r, 0)), device_id_type=MESH,
        )

    def xy_copy(j, r):
        py = lax.rem(y + r, 4)
        return pltpu.make_async_remote_copy(
            src_ref=mid_x.at[j, py], dst_ref=in_xy.at[j, r - 1],
            send_sem=xy_out.at[j, r - 1], recv_sem=xy_in.at[j, r - 1],
            device_id=(z, device(0, r, 0)), device_id_type=MESH,
        )

    def yx_copy(j, r):
        px = lax.rem(x + r, 4)
        return pltpu.make_async_remote_copy(
            src_ref=mid_y.at[j, px], dst_ref=in_yx.at[j, r - 1],
            send_sem=yx_out.at[j, r - 1], recv_sem=yx_in.at[j, r - 1],
            device_id=(z, device(r, 0, 0)), device_id_type=MESH,
        )

    def z_copy(j, a, slot):
        return pltpu.make_async_remote_copy(
            src_ref=last.at[j, a], dst_ref=in_z.at[slot],
            send_sem=z_out.at[j, a], recv_sem=z_in.at[slot],
            device_id=(2 * j + a, me), device_id_type=MESH,
        )

    def cross(j, h):
        at = h * 256
        rows = jnp.dot(turned[at : at + 256, :], weight[j % 2], preferred_element_type=F32)
        sent[j, :, :, :, at : at + 256] = rows.astype(BF16).T.reshape(4, 4, 16, 256)

    def travel(j):
        for r in (2, 1, 3):
            x_copy(j, r).start()
            y_copy(j, r).start()

    def second(j):
        for r in (1, 3, 2):
            x_copy(j, r).wait_recv()
        total = sent[j, x, :, :, 0:256].astype(F32)
        for r in range(3):
            total = total + in_x[j, r].astype(F32)
        mid_x[j] = total
        for r in (1, 3, 2):
            y_copy(j, r).wait_recv()
        for r in (2, 1, 3):
            xy_copy(j, r).start()
        total = sent[j, :, y, :, 256:512].astype(F32)
        for r in range(3):
            total = total + in_y[j, r].astype(F32)
        mid_y[j] = total
        for r in (2, 1, 3):
            yx_copy(j, r).start()

    def third(j):
        for r in (1, 3, 2):
            xy_copy(j, r).wait_recv()
        one = mid_x[j, y]
        for r in range(3):
            one = one + in_xy[j, r]
        for r in (1, 3, 2):
            yx_copy(j, r).wait_recv()
        two = mid_y[j, x]
        for r in range(3):
            two = two + in_yx[j, r]
        for a in range(2):
            last[j, a, :, 0:256] = one[a * 8 : a * 8 + 8]
            last[j, a, :, 256:512] = two[a * 8 : a * 8 + 8]
        for a in range(2):
            @pl.when(z != 2 * j + a)
            def _():
                z_copy(j, a, lax.rem(z - (2 * j + a) + 8, 8) - 1).start()

    for g in range(4):
        normalise(g, 0)
    give.wait_recv()
    for g in range(4):
        normalise(g, 1)
        if g:
            turn_over(g - 1)
            weigh(0, (g - 1) * 640, 640)
    turn_over(3)
    weigh(0, 1920, 640)
    for j in range(1, CHUNKS + 1):
        for h in range(2):
            if j < CHUNKS:
                weigh(j, h * 1280, 640)
                weigh(j, h * 1280 + 640, 640)
            cross(j - 1, h)
        if j == CHUNKS:
            second(0)
        travel(j - 1)
    give.wait_send()
    for d in others:
        stat_copy(d).wait_send()
    for j in range(1, CHUNKS):
        second(j)
    for j in range(CHUNKS):
        for r in (1, 2, 3):
            x_copy(j, r).wait_send()
            y_copy(j, r).wait_send()
    for j in range(CHUNKS):
        third(j)

    for j in range(CHUNKS):
        for r in (1, 2, 3):
            xy_copy(j, r).wait_send()
            yx_copy(j, r).wait_send()
    for slot in range(7):
        z_copy(0, 0, slot).wait_recv()
    total = last[lax.div(z, 2), lax.rem(z, 2)]
    for slot in range(7):
        total = total + in_z[slot]
    at = pl.multiple_of((x * 4 + y) * 16 + lax.rem(z, 2) * 8, 8)
    out[...] = own_load[lax.div(z, 2), pl.ds(at, 8), :] * total / (tails * paths)

    for j in range(CHUNKS):
        for a in range(2):
            @pl.when(z != 2 * j + a)
            def _():
                z_copy(j, a, 0).wait_send()


def body(normals, states, loadings, strikes, hedge, sigma, tail):
    nodes, per_node, factors = normals.shape
    rows = CAP * per_node * 2
    dma = pltpu.SemaphoreType.DMA
    return pl.pallas_call(
        kernel,
        out_shape=jax.ShapeDtypeStruct((8, factors), F32),
        in_specs=[pl.BlockSpec(memory_space=pltpu.HBM)] * 7,
        out_specs=pl.BlockSpec(memory_space=pltpu.VMEM),
        scratch_shapes=[
            pltpu.VMEM(normals.shape, BF16),
            pltpu.VMEM((CAP, per_node, factors), BF16),
            pltpu.VMEM((CAP, per_node, factors), BF16),
            pltpu.VMEM(loadings.shape, BF16),
            pltpu.VMEM(states.shape, BF16),
            pltpu.VMEM((4, nodes, 128), F32),
            pltpu.VMEM((8, 256), F32),
            pltpu.VMEM((8, 256), F32),
            pltpu.VMEM((1, factors), F32),
            pltpu.VMEM((4, 1, 128), F32),
            pltpu.SMEM(tail.shape, jnp.int32),
            pltpu.SMEM((CAP,), jnp.int32),
            pltpu.SMEM((CAP,), F32),
            pltpu.VMEM((2, 16, 5, 4, 128), F32),
            pltpu.VMEM((16, 5, 4, 128), F32),
            pltpu.VMEM((16, 5, 4, 128), F32),
            pltpu.VMEM((16, 5, 4, 128), F32),
            pltpu.VMEM((2, 16, 5, 4, 128), F32),
            pltpu.VMEM((CHUNKS, 1, 256), F32),
            pltpu.VMEM((CHUNKS, 1, 256), F32),
            pltpu.VMEM((CHUNKS, 256, factors), F32),
            pltpu.VMEM((CHUNKS, factors, 256), BF16),
            pltpu.VMEM((rows, factors), BF16),
            pltpu.VMEM((rows, factors), BF16),
            pltpu.VMEM((factors, rows), BF16),
            pltpu.VMEM((2, rows, 256), BF16),
            pltpu.VMEM((CHUNKS, 4, 4, 16, factors), BF16),
            pltpu.VMEM((CHUNKS, 3, 4, 16, 256), BF16),
            pltpu.VMEM((CHUNKS, 3, 4, 16, 256), BF16),
            pltpu.VMEM((CHUNKS, 4, 16, 256), F32),
            pltpu.VMEM((CHUNKS, 4, 16, 256), F32),
            pltpu.VMEM((CHUNKS, 3, 16, 256), F32),
            pltpu.VMEM((CHUNKS, 3, 16, 256), F32),
            pltpu.VMEM((CHUNKS, 2, 8, factors), F32),
            pltpu.VMEM((7, 8, factors), F32),
            dma((21,)),
            dma((2,)),
            dma((2,)),
            dma((2,)),
            dma((16,)),
            dma((16,)),
            dma((16,)),
            dma((16,)),
            dma((CHUNKS, 3)),
            dma((CHUNKS, 3)),
            dma((CHUNKS, 3)),
            dma((CHUNKS, 3)),
            dma((CHUNKS, 3)),
            dma((CHUNKS, 3)),
            dma((CHUNKS, 3)),
            dma((CHUNKS, 3)),
            dma((CHUNKS, 2)),
            dma((7,)),
        ],
        compiler_params=pltpu.CompilerParams(
            collective_id=0, has_side_effects=True, vmem_limit_bytes=63 * 1024 * 1024
        ),
    )(
        normals, states, loadings, strikes, hedge, sigma.reshape(1, factors), tail,
    )


def solution(mesh):
    in_specs = (P("outer", "inner", None), P("outer", None), P(), P(), P(), P(), P())
    out_specs = P(("outer", "inner"), None)
    return jax.shard_map(body, mesh=mesh, in_specs=in_specs, out_specs=out_specs, check_vma=False)
```

```python
import jax
import jax.numpy as jnp
from jax import lax
from jax.experimental import pallas as pl
from jax.experimental.pallas import tpu as pltpu
from jax.sharding import PartitionSpec as P

CAP = 80
EPSILON = 1e-06
CHUNKS = 4
MESH = pl.DeviceIdType.MESH
F32 = jnp.float32
BF16 = jnp.bfloat16


def place(hit):
    return jnp.where(hit, 1.0, 0.0)


def offsets():
    span = (0, 1, 2, 1)
    every = [(dx, dy) for dx in range(4) for dy in range(4)][1:]
    return sorted(every, key=lambda d: -(span[d[0]] + span[d[1]]))


def kernel(
    normals, states, loadings, strikes, hedge, sigma, tail, out,
    held, own, pair, load_v, states_b, states_f, strikes_v, hedge_v, sigma_v, sigma_f, tail_s, slot_s, live_s,
    sums, sums_pair, sums_chip, sums_in, stats, half_strike, half_hedge, own_load, load_t,
    mixed, part, turned, weight, sent, in_x, in_y, mid_x, mid_y, in_xy, in_yx, last, in_z,
    copy_sem, pair_sem, join_sem, pass_sem, sum_out, sum_in, stat_out, stat_in,
    x_out, x_in, y_out, y_in, xy_out, xy_in, yx_out, yx_in, z_out, z_in,
):
    z = lax.axis_index("outer")
    me = lax.axis_index("inner")
    x, y, c = lax.div(me, 8), lax.rem(lax.div(me, 2), 4), lax.rem(me, 2)
    nodes, per_node, factors = held.shape
    paths = per_node * 32
    tails = tail_s.shape[0]
    others = offsets()

    def device(dx, dy, dc):
        return (lax.rem(x + dx, 4) * 4 + lax.rem(y + dy, 4)) * 2 + lax.rem(c + dc, 2)

    copies = [
        (tail, tail_s), (normals, held), (states, states_b), (sigma, sigma_v), (loadings, load_v),
    ]
    for i in range(8):
        copies.append((strikes.at[pl.ds(i * 256, 256)], strikes_v.at[i]))
        copies.append((hedge.at[pl.ds(i * 256, 256)], hedge_v.at[i]))
    loads = [pltpu.make_async_copy(a, b, copy_sem.at[i]) for i, (a, b) in enumerate(copies)]
    loads[0].start()
    loads[1].start()

    barrier = pltpu.get_barrier_semaphore()

    def greet(where):
        pl.semaphore_signal(barrier, inc=1, device_id=where, device_id_type=MESH)

    for dx, dy in others:
        greet((z, device(dx, dy, 0)))
    for d in (4, 3, 5, 2, 6, 1, 7):
        greet((lax.rem(z + d, 8), me))
    partner = (z, device(0, 0, 1))
    greet(partner)
    for item in loads[2:]:
        item.start()

    loads[0].wait()
    first = jnp.int32(0)
    step = tails // 2
    while step:
        first = first + jnp.where(tail_s[first + step - 1] < z * nodes, step, 0)
        step //= 2

    def find(s, carry):
        at = jnp.minimum(first + s, tails - 1)
        node = tail_s[at] - z * nodes
        good = (first + s < tails) & (node >= 0) & (node < nodes)
        slot_s[s] = jnp.clip(node, 0, nodes - 1)
        live_s[s] = jnp.where(good, 1.0, 0.0).astype(F32)
        return carry

    lax.fori_loop(0, CAP, find, 0, unroll=8)
    loads[1].wait()

    def add_up(q, carry):
        for i in range(5):
            rows = held[slot_s[q * 5 + i]]
            own[q * 5 + i] = rows
            block = rows.astype(F32)
            one = jnp.sum(block, axis=0, keepdims=True)
            two = jnp.sum(block * block, axis=0, keepdims=True)
            for h in range(2):
                for b in range(2):
                    lanes = slice(h * 256 + b * 128, h * 256 + b * 128 + 128)
                    sums[h, q, i, b : b + 1, :] = one[:, lanes]
                    sums[h, q, i, 2 + b : 3 + b, :] = two[:, lanes]
        return carry

    lax.fori_loop(0, 16, add_up, 0)
    pl.semaphore_wait(barrier, 23)

    join = pltpu.make_async_remote_copy(
        src_ref=sums.at[1 - c], dst_ref=sums_pair, send_sem=join_sem.at[0], recv_sem=join_sem.at[1],
        device_id=partner, device_id_type=MESH,
    )
    join.start()
    for item in loads[2:]:
        item.wait()
    for b in range(4):
        lanes = slice(b * 128, b * 128 + 128)
        states_f[b] = states_b[:, lanes].astype(F32)
        sigma_f[b] = sigma_v[:, lanes]
    join.wait_recv()
    sums_chip[...] = sums[c] + sums_pair[...]

    def sum_copy(d):
        dx, dy = d
        return pltpu.make_async_remote_copy(
            src_ref=sums_chip.at[lax.rem(x + dx, 4) * 4 + lax.rem(y + dy, 4)],
            dst_ref=sums_in.at[dx * 4 + dy],
            send_sem=sum_out.at[dx * 4 + dy], recv_sem=sum_in.at[dx * 4 + dy],
            device_id=(z, device(dx, dy, 0)), device_id_type=MESH,
        )

    def stat_copy(d):
        dx, dy = d
        return pltpu.make_async_remote_copy(
            src_ref=stats.at[0, 0], dst_ref=stats.at[0, dx * 4 + dy],
            send_sem=stat_out.at[dx * 4 + dy], recv_sem=stat_in.at[dx * 4 + dy],
            device_id=(z, device(dx, dy, 0)), device_id_type=MESH,
        )

    for d in others:
        sum_copy(d).start()
    swap = pltpu.make_async_remote_copy(
        src_ref=own, dst_ref=pair, send_sem=pair_sem.at[0], recv_sem=pair_sem.at[1],
        device_id=partner, device_id_type=MESH,
    )
    swap.start()

    m_id = lax.broadcasted_iota(jnp.int32, (256, 256), 0)
    l_id = lax.broadcasted_iota(jnp.int32, (256, 256), 1)
    same = (m_id // 16 == l_id // 16) & (m_id % 8 == l_id % 8)
    picks = [same & ((m_id // 8) % 2 == c) & ((l_id // 8) % 2 == a) for a in range(2)]
    picks_t = [same & ((l_id // 8) % 2 == c) & ((m_id // 8) % 2 == a) for a in range(2)]
    for source, target in ((strikes_v, half_strike), (hedge_v, half_hedge)):
        rows = source[...] * 0.5
        moved = [
            jnp.dot(rows, place(pick), precision=lax.Precision.HIGHEST, preferred_element_type=F32)
            for pick in picks
        ]
        for j in range(CHUNKS):
            target[j] = moved[0][2 * j : 2 * j + 1] + moved[1][2 * j + 1 : 2 * j + 2]
    turn = [place(pick).astype(BF16) for pick in picks_t]

    def order(j, carry):
        rows = jnp.zeros((256, factors), F32)
        for a in range(2):
            at = pl.multiple_of((2 * j + a) * 256, 256)
            rows = rows + jnp.dot(turn[a], load_v[pl.ds(at, 256), :], preferred_element_type=F32)
        own_load[j] = rows
        load_t[j] = (rows * 0.5).astype(BF16).T
        return carry

    lax.fori_loop(0, CHUNKS, order, 0)

    total = sums_chip[x * 4 + y]
    for d in reversed(others):
        sum_copy(d).wait_recv()
        total = total + sums_in[d[0] * 4 + d[1]]
    center = total[:, 0:2, :] / paths
    spread = total[:, 2:4, :] / paths - center * center
    stats[0, 0, :, 0:2, :] = center
    stats[0, 0, :, 2:4, :] = lax.rsqrt(spread + EPSILON)
    for d in others:
        stat_copy(d).start()
    for d in others:
        sum_copy(d).wait_send()
    join.wait_send()
    swap.wait()
    for d in reversed(others):
        stat_copy(d).wait_recv()
    give = pltpu.make_async_remote_copy(
        src_ref=stats.at[0], dst_ref=stats.at[1], send_sem=pass_sem.at[0], recv_sem=pass_sem.at[1],
        device_id=partner, device_id_type=MESH,
    )
    give.start()

    def normalise(g, e):
        base = (c if e == 0 else 1 - c) * 2
        for dy in range(4):
            q = lax.rem(x + 4 - g, 4) * 4 + lax.rem(y + 4 - dy, 4)
            for i in range(5):
                s = q * 5 + i
                at, live = slot_s[s], live_s[s]
                for b in range(2):
                    lanes = pl.ds(pl.multiple_of((base + b) * 128, 128), 128)
                    state = states_f[base + b, pl.ds(at, 1), :]
                    mean = stats[e, g * 4 + dy, i, b : b + 1, :]
                    scale = stats[e, g * 4 + dy, i, 2 + b : 3 + b, :] * live
                    for w, source in enumerate((own, pair)):
                        row = (g * 4 + dy) * 160 + i * 32 + w * 16
                        block = source[s, :, lanes].astype(F32)
                        scaled = ((block - mean) * scale).astype(BF16)
                        both = state + sigma_f[base + b] * scaled.astype(F32)
                        mixed[row : row + 16, lanes] = both.astype(BF16)
                        part[row : row + 16, lanes] = scaled

    def turn_over(g):
        for b in range(5):
            at = g * 640 + b * 128
            turned[:, at : at + 128] = part[at : at + 128, :].T

    def weigh(j, at, count):
        level = jnp.dot(mixed[at : at + count, :], load_t[j], preferred_element_type=F32)
        size = half_hedge[j]
        fresh = size + size * jnp.tanh(level - half_strike[j])
        weight[j % 2, at : at + count, :] = fresh.astype(BF16)

    def x_copy(j, r):
        px = lax.rem(x + r, 4)
        return pltpu.make_async_remote_copy(
            src_ref=sent.at[j, px, :, :, pl.ds(0, 256)], dst_ref=in_x.at[j, r - 1],
            send_sem=x_out.at[j, r - 1], recv_sem=x_in.at[j, r - 1],
            device_id=(z, device(r, 0, 0)), device_id_type=MESH,
        )

    def y_copy(j, r):
        py = lax.rem(y + r, 4)
        return pltpu.make_async_remote_copy(
            src_ref=sent.at[j, :, py, :, pl.ds(256, 256)], dst_ref=in_y.at[j, r - 1],
            send_sem=y_out.at[j, r - 1], recv_sem=y_in.at[j, r - 1],
            device_id=(z, device(0, r, 0)), device_id_type=MESH,
        )

    def xy_copy(j, r):
        py = lax.rem(y + r, 4)
        return pltpu.make_async_remote_copy(
            src_ref=mid_x.at[j, py], dst_ref=in_xy.at[j, r - 1],
            send_sem=xy_out.at[j, r - 1], recv_sem=xy_in.at[j, r - 1],
            device_id=(z, device(0, r, 0)), device_id_type=MESH,
        )

    def yx_copy(j, r):
        px = lax.rem(x + r, 4)
        return pltpu.make_async_remote_copy(
            src_ref=mid_y.at[j, px], dst_ref=in_yx.at[j, r - 1],
            send_sem=yx_out.at[j, r - 1], recv_sem=yx_in.at[j, r - 1],
            device_id=(z, device(r, 0, 0)), device_id_type=MESH,
        )

    def z_copy(j, a, slot):
        return pltpu.make_async_remote_copy(
            src_ref=last.at[j, a], dst_ref=in_z.at[slot],
            send_sem=z_out.at[j, a], recv_sem=z_in.at[slot],
            device_id=(2 * j + a, me), device_id_type=MESH,
        )

    def cross(j, h):
        at = h * 256
        rows = jnp.dot(turned[at : at + 256, :], weight[j % 2], preferred_element_type=F32)
        sent[j, :, :, :, at : at + 256] = rows.astype(BF16).T.reshape(4, 4, 16, 256)

    def travel(j):
        for r in (2, 1, 3):
            x_copy(j, r).start()
            y_copy(j, r).start()

    def second(j):
        for r in (1, 3, 2):
            x_copy(j, r).wait_recv()
        total = sent[j, x, :, :, 0:256].astype(F32)
        for r in range(3):
            total = total + in_x[j, r].astype(F32)
        mid_x[j] = total
        for r in (1, 3, 2):
            y_copy(j, r).wait_recv()
        for r in (2, 1, 3):
            xy_copy(j, r).start()
        total = sent[j, :, y, :, 256:512].astype(F32)
        for r in range(3):
            total = total + in_y[j, r].astype(F32)
        mid_y[j] = total
        for r in (2, 1, 3):
            yx_copy(j, r).start()

    def third(j):
        for r in (1, 3, 2):
            xy_copy(j, r).wait_recv()
        one = mid_x[j, y]
        for r in range(3):
            one = one + in_xy[j, r]
        for r in (1, 3, 2):
            yx_copy(j, r).wait_recv()
        two = mid_y[j, x]
        for r in range(3):
            two = two + in_yx[j, r]
        for a in range(2):
            last[j, a, :, 0:256] = one[a * 8 : a * 8 + 8]
            last[j, a, :, 256:512] = two[a * 8 : a * 8 + 8]
        for a in range(2):
            @pl.when(z != 2 * j + a)
            def _():
                z_copy(j, a, lax.rem(z - (2 * j + a) + 8, 8) - 1).start()

    for g in range(4):
        normalise(g, 0)
    give.wait_recv()
    for g in range(4):
        normalise(g, 1)
        if g:
            turn_over(g - 1)
            weigh(0, (g - 1) * 640, 640)
    turn_over(3)
    weigh(0, 1920, 640)
    for j in range(1, CHUNKS + 1):
        for h in range(2):
            if j < CHUNKS:
                weigh(j, h * 1280, 640)
                weigh(j, h * 1280 + 640, 640)
            cross(j - 1, h)
        if j == CHUNKS:
            second(0)
        travel(j - 1)
    give.wait_send()
    for d in others:
        stat_copy(d).wait_send()
    for j in range(1, CHUNKS):
        second(j)
    for j in range(CHUNKS):
        for r in (1, 2, 3):
            x_copy(j, r).wait_send()
            y_copy(j, r).wait_send()
    for j in range(CHUNKS):
        third(j)

    for j in range(CHUNKS):
        for r in (1, 2, 3):
            xy_copy(j, r).wait_send()
            yx_copy(j, r).wait_send()
    for slot in range(7):
        z_copy(0, 0, slot).wait_recv()
    total = last[lax.div(z, 2), lax.rem(z, 2)]
    for slot in range(7):
        total = total + in_z[slot]
    at = pl.multiple_of((x * 4 + y) * 16 + lax.rem(z, 2) * 8, 8)
    out[...] = own_load[lax.div(z, 2), pl.ds(at, 8), :] * total / (tails * paths)

    for j in range(CHUNKS):
        for a in range(2):
            @pl.when(z != 2 * j + a)
            def _():
                z_copy(j, a, 0).wait_send()


def body(normals, states, loadings, strikes, hedge, sigma, tail):
    nodes, per_node, factors = normals.shape
    rows = CAP * per_node * 2
    dma = pltpu.SemaphoreType.DMA
    return pl.pallas_call(
        kernel,
        out_shape=pltpu.VMEM((8, factors), F32),
        in_specs=[pl.BlockSpec(memory_space=pltpu.HBM)] * 7,
        out_specs=pl.BlockSpec(memory_space=pltpu.VMEM),
        scratch_shapes=[
            pltpu.VMEM(normals.shape, BF16),
            pltpu.VMEM((CAP, per_node, factors), BF16),
            pltpu.VMEM((CAP, per_node, factors), BF16),
            pltpu.VMEM(loadings.shape, BF16),
            pltpu.VMEM(states.shape, BF16),
            pltpu.VMEM((4, nodes, 128), F32),
            pltpu.VMEM((8, 256), F32),
            pltpu.VMEM((8, 256), F32),
            pltpu.VMEM((1, factors), F32),
            pltpu.VMEM((4, 1, 128), F32),
            pltpu.SMEM(tail.shape, jnp.int32),
            pltpu.SMEM((CAP,), jnp.int32),
            pltpu.SMEM((CAP,), F32),
            pltpu.VMEM((2, 16, 5, 4, 128), F32),
            pltpu.VMEM((16, 5, 4, 128), F32),
            pltpu.VMEM((16, 5, 4, 128), F32),
            pltpu.VMEM((16, 5, 4, 128), F32),
            pltpu.VMEM((2, 16, 5, 4, 128), F32),
            pltpu.VMEM((CHUNKS, 1, 256), F32),
            pltpu.VMEM((CHUNKS, 1, 256), F32),
            pltpu.VMEM((CHUNKS, 256, factors), F32),
            pltpu.VMEM((CHUNKS, factors, 256), BF16),
            pltpu.VMEM((rows, factors), BF16),
            pltpu.VMEM((rows, factors), BF16),
            pltpu.VMEM((factors, rows), BF16),
            pltpu.VMEM((2, rows, 256), BF16),
            pltpu.VMEM((CHUNKS, 4, 4, 16, factors), BF16),
            pltpu.VMEM((CHUNKS, 3, 4, 16, 256), BF16),
            pltpu.VMEM((CHUNKS, 3, 4, 16, 256), BF16),
            pltpu.VMEM((CHUNKS, 4, 16, 256), F32),
            pltpu.VMEM((CHUNKS, 4, 16, 256), F32),
            pltpu.VMEM((CHUNKS, 3, 16, 256), F32),
            pltpu.VMEM((CHUNKS, 3, 16, 256), F32),
            pltpu.VMEM((CHUNKS, 2, 8, factors), F32),
            pltpu.VMEM((7, 8, factors), F32),
            dma((21,)),
            dma((2,)),
            dma((2,)),
            dma((2,)),
            dma((16,)),
            dma((16,)),
            dma((16,)),
            dma((16,)),
            dma((CHUNKS, 3)),
            dma((CHUNKS, 3)),
            dma((CHUNKS, 3)),
            dma((CHUNKS, 3)),
            dma((CHUNKS, 3)),
            dma((CHUNKS, 3)),
            dma((CHUNKS, 3)),
            dma((CHUNKS, 3)),
            dma((CHUNKS, 2)),
            dma((7,)),
        ],
        compiler_params=pltpu.CompilerParams(
            collective_id=0, has_side_effects=True, vmem_limit_bytes=63 * 1024 * 1024
        ),
    )(
        normals, states, loadings, strikes, hedge, sigma.reshape(1, factors), tail,
    )


def solution(mesh):
    in_specs = (P("outer", "inner", None), P("outer", None), P(), P(), P(), P(), P())
    out_specs = P(("outer", "inner"), None)
    return jax.shard_map(body, mesh=mesh, in_specs=in_specs, out_specs=out_specs, check_vma=False)
```

```python
import jax
import jax.numpy as jnp
from jax import lax
from jax.experimental import pallas as pl
from jax.experimental.pallas import tpu as pltpu
from jax.sharding import PartitionSpec as P

CAP = 80
EPSILON = 1e-06
CHUNKS = 4
MESH = pl.DeviceIdType.MESH
F32 = jnp.float32
BF16 = jnp.bfloat16


def place(hit):
    return jnp.where(hit, 1.0, 0.0)


def offsets():
    span = (0, 1, 2, 1)
    every = [(dx, dy) for dx in range(4) for dy in range(4)][1:]
    return sorted(every, key=lambda d: -(span[d[0]] + span[d[1]]))


def kernel(
    normals, states, loadings, strikes, hedge, sigma, tail, out,
    held, own, pair, load_v, states_b, states_f, strikes_v, hedge_v, sigma_v, sigma_f, tail_s, slot_s, live_s,
    sums, sums_pair, sums_chip, sums_in, stats, half_strike, half_hedge, own_load, load_t,
    mixed, part, turned, weight, sent, in_x, in_y, mid_x, mid_y, in_xy, in_yx, last, in_z,
    copy_sem, pair_sem, join_sem, pass_sem, sum_out, sum_in, stat_out, stat_in,
    x_out, x_in, y_out, y_in, xy_out, xy_in, yx_out, yx_in, z_out, z_in,
):
    z = lax.axis_index("outer")
    me = lax.axis_index("inner")
    x, y, c = lax.div(me, 8), lax.rem(lax.div(me, 2), 4), lax.rem(me, 2)
    nodes, per_node, factors = held.shape
    paths = per_node * 32
    tails = tail_s.shape[0]
    others = offsets()

    def device(dx, dy, dc):
        return (lax.rem(x + dx, 4) * 4 + lax.rem(y + dy, 4)) * 2 + lax.rem(c + dc, 2)

    copies = [
        (tail, tail_s), (normals, held), (states, states_b), (sigma, sigma_v), (loadings, load_v),
    ]
    for i in range(8):
        copies.append((strikes.at[pl.ds(i * 256, 256)], strikes_v.at[i]))
        copies.append((hedge.at[pl.ds(i * 256, 256)], hedge_v.at[i]))
    loads = [pltpu.make_async_copy(a, b, copy_sem.at[i]) for i, (a, b) in enumerate(copies)]
    loads[0].start()
    loads[1].start()

    barrier = pltpu.get_barrier_semaphore()

    def greet(where):
        pl.semaphore_signal(barrier, inc=1, device_id=where, device_id_type=MESH)

    for dx, dy in others:
        greet((z, device(dx, dy, 0)))
    for d in (4, 3, 5, 2, 6, 1, 7):
        greet((lax.rem(z + d, 8), me))
    partner = (z, device(0, 0, 1))
    greet(partner)
    loads[0].wait()
    first = jnp.int32(0)
    step = tails // 2
    while step:
        first = first + jnp.where(tail_s[first + step - 1] < z * nodes, step, 0)
        step //= 2

    def find(s, carry):
        at = jnp.minimum(first + s, tails - 1)
        node = tail_s[at] - z * nodes
        good = (first + s < tails) & (node >= 0) & (node < nodes)
        slot_s[s] = jnp.clip(node, 0, nodes - 1)
        live_s[s] = jnp.where(good, 1.0, 0.0).astype(F32)
        return carry

    lax.fori_loop(0, CAP, find, 0, unroll=8)
    loads[1].wait()
    for item in loads[2:]:
        item.start()

    def add_up(q, carry):
        for i in range(5):
            rows = held[slot_s[q * 5 + i]]
            own[q * 5 + i] = rows
            block = rows.astype(F32)
            one = jnp.sum(block, axis=0, keepdims=True)
            two = jnp.sum(block * block, axis=0, keepdims=True)
            for h in range(2):
                for b in range(2):
                    lanes = slice(h * 256 + b * 128, h * 256 + b * 128 + 128)
                    sums[h, q, i, b : b + 1, :] = one[:, lanes]
                    sums[h, q, i, 2 + b : 3 + b, :] = two[:, lanes]
        return carry

    lax.fori_loop(0, 16, add_up, 0)
    pl.semaphore_wait(barrier, 23)

    join = pltpu.make_async_remote_copy(
        src_ref=sums.at[1 - c], dst_ref=sums_pair, send_sem=join_sem.at[0], recv_sem=join_sem.at[1],
        device_id=partner, device_id_type=MESH,
    )
    join.start()
    for item in loads[2:]:
        item.wait()
    for b in range(4):
        lanes = slice(b * 128, b * 128 + 128)
        states_f[b] = states_b[:, lanes].astype(F32)
        sigma_f[b] = sigma_v[:, lanes]
    join.wait_recv()
    sums_chip[...] = sums[c] + sums_pair[...]

    def sum_copy(d):
        dx, dy = d
        return pltpu.make_async_remote_copy(
            src_ref=sums_chip.at[lax.rem(x + dx, 4) * 4 + lax.rem(y + dy, 4)],
            dst_ref=sums_in.at[dx * 4 + dy],
            send_sem=sum_out.at[dx * 4 + dy], recv_sem=sum_in.at[dx * 4 + dy],
            device_id=(z, device(dx, dy, 0)), device_id_type=MESH,
        )

    def stat_copy(d):
        dx, dy = d
        return pltpu.make_async_remote_copy(
            src_ref=stats.at[0, 0], dst_ref=stats.at[0, dx * 4 + dy],
            send_sem=stat_out.at[dx * 4 + dy], recv_sem=stat_in.at[dx * 4 + dy],
            device_id=(z, device(dx, dy, 0)), device_id_type=MESH,
        )

    for d in others:
        sum_copy(d).start()
    swap = pltpu.make_async_remote_copy(
        src_ref=own, dst_ref=pair, send_sem=pair_sem.at[0], recv_sem=pair_sem.at[1],
        device_id=partner, device_id_type=MESH,
    )
    swap.start()

    m_id = lax.broadcasted_iota(jnp.int32, (256, 256), 0)
    l_id = lax.broadcasted_iota(jnp.int32, (256, 256), 1)
    same = (m_id // 16 == l_id // 16) & (m_id % 8 == l_id % 8)
    picks = [same & ((m_id // 8) % 2 == c) & ((l_id // 8) % 2 == a) for a in range(2)]
    picks_t = [same & ((l_id // 8) % 2 == c) & ((m_id // 8) % 2 == a) for a in range(2)]
    for source, target in ((strikes_v, half_strike), (hedge_v, half_hedge)):
        rows = source[...] * 0.5
        moved = [
            jnp.dot(rows, place(pick), precision=lax.Precision.HIGHEST, preferred_element_type=F32)
            for pick in picks
        ]
        for j in range(CHUNKS):
            target[j] = moved[0][2 * j : 2 * j + 1] + moved[1][2 * j + 1 : 2 * j + 2]
    turn = [place(pick).astype(BF16) for pick in picks_t]

    def order(j, carry):
        rows = jnp.zeros((256, factors), F32)
        for a in range(2):
            at = pl.multiple_of((2 * j + a) * 256, 256)
            rows = rows + jnp.dot(turn[a], load_v[pl.ds(at, 256), :], preferred_element_type=F32)
        own_load[j] = rows
        load_t[j] = (rows * 0.5).astype(BF16).T
        return carry

    lax.fori_loop(0, CHUNKS, order, 0)

    total = sums_chip[x * 4 + y]
    for d in reversed(others):
        sum_copy(d).wait_recv()
        total = total + sums_in[d[0] * 4 + d[1]]
    center = total[:, 0:2, :] / paths
    spread = total[:, 2:4, :] / paths - center * center
    stats[0, 0, :, 0:2, :] = center
    stats[0, 0, :, 2:4, :] = lax.rsqrt(spread + EPSILON)
    for d in others:
        stat_copy(d).start()
    for d in others:
        sum_copy(d).wait_send()
    join.wait_send()
    swap.wait()
    for d in reversed(others):
        stat_copy(d).wait_recv()
    give = pltpu.make_async_remote_copy(
        src_ref=stats.at[0], dst_ref=stats.at[1], send_sem=pass_sem.at[0], recv_sem=pass_sem.at[1],
        device_id=partner, device_id_type=MESH,
    )
    give.start()

    def normalise(g, e):
        base = (c if e == 0 else 1 - c) * 2
        for dy in range(4):
            q = lax.rem(x + 4 - g, 4) * 4 + lax.rem(y + 4 - dy, 4)
            for i in range(5):
                s = q * 5 + i
                at, live = slot_s[s], live_s[s]
                for b in range(2):
                    lanes = pl.ds(pl.multiple_of((base + b) * 128, 128), 128)
                    state = states_f[base + b, pl.ds(at, 1), :]
                    mean = stats[e, g * 4 + dy, i, b : b + 1, :]
                    scale = stats[e, g * 4 + dy, i, 2 + b : 3 + b, :] * live
                    for w, source in enumerate((own, pair)):
                        row = (g * 4 + dy) * 160 + i * 32 + w * 16
                        block = source[s, :, lanes].astype(F32)
                        scaled = ((block - mean) * scale).astype(BF16)
                        both = state + sigma_f[base + b] * scaled.astype(F32)
                        mixed[row : row + 16, lanes] = both.astype(BF16)
                        part[row : row + 16, lanes] = scaled

    def turn_over(g):
        for b in range(5):
            at = g * 640 + b * 128
            turned[:, at : at + 128] = part[at : at + 128, :].T

    def weigh(j, at, count):
        level = jnp.dot(mixed[at : at + count, :], load_t[j], preferred_element_type=F32)
        size = half_hedge[j]
        fresh = size + size * jnp.tanh(level - half_strike[j])
        weight[j % 2, at : at + count, :] = fresh.astype(BF16)

    def x_copy(j, r):
        px = lax.rem(x + r, 4)
        return pltpu.make_async_remote_copy(
            src_ref=sent.at[j, px, :, :, pl.ds(0, 256)], dst_ref=in_x.at[j, r - 1],
            send_sem=x_out.at[j, r - 1], recv_sem=x_in.at[j, r - 1],
            device_id=(z, device(r, 0, 0)), device_id_type=MESH,
        )

    def y_copy(j, r):
        py = lax.rem(y + r, 4)
        return pltpu.make_async_remote_copy(
            src_ref=sent.at[j, :, py, :, pl.ds(256, 256)], dst_ref=in_y.at[j, r - 1],
            send_sem=y_out.at[j, r - 1], recv_sem=y_in.at[j, r - 1],
            device_id=(z, device(0, r, 0)), device_id_type=MESH,
        )

    def xy_copy(j, r):
        py = lax.rem(y + r, 4)
        return pltpu.make_async_remote_copy(
            src_ref=mid_x.at[j, py], dst_ref=in_xy.at[j, r - 1],
            send_sem=xy_out.at[j, r - 1], recv_sem=xy_in.at[j, r - 1],
            device_id=(z, device(0, r, 0)), device_id_type=MESH,
        )

    def yx_copy(j, r):
        px = lax.rem(x + r, 4)
        return pltpu.make_async_remote_copy(
            src_ref=mid_y.at[j, px], dst_ref=in_yx.at[j, r - 1],
            send_sem=yx_out.at[j, r - 1], recv_sem=yx_in.at[j, r - 1],
            device_id=(z, device(r, 0, 0)), device_id_type=MESH,
        )

    def z_copy(j, a, slot):
        return pltpu.make_async_remote_copy(
            src_ref=last.at[j, a], dst_ref=in_z.at[slot],
            send_sem=z_out.at[j, a], recv_sem=z_in.at[slot],
            device_id=(2 * j + a, me), device_id_type=MESH,
        )

    def cross(j, h):
        at = h * 256
        rows = jnp.dot(turned[at : at + 256, :], weight[j % 2], preferred_element_type=F32)
        sent[j, :, :, :, at : at + 256] = rows.astype(BF16).T.reshape(4, 4, 16, 256)

    def travel(j):
        for r in (2, 1, 3):
            x_copy(j, r).start()
            y_copy(j, r).start()

    def second(j):
        for r in (1, 3, 2):
            x_copy(j, r).wait_recv()
        total = sent[j, x, :, :, 0:256].astype(F32)
        for r in range(3):
            total = total + in_x[j, r].astype(F32)
        mid_x[j] = total
        for r in (1, 3, 2):
            y_copy(j, r).wait_recv()
        for r in (2, 1, 3):
            xy_copy(j, r).start()
        total = sent[j, :, y, :, 256:512].astype(F32)
        for r in range(3):
            total = total + in_y[j, r].astype(F32)
        mid_y[j] = total
        for r in (2, 1, 3):
            yx_copy(j, r).start()

    def third(j):
        for r in (1, 3, 2):
            xy_copy(j, r).wait_recv()
        one = mid_x[j, y]
        for r in range(3):
            one = one + in_xy[j, r]
        for r in (1, 3, 2):
            yx_copy(j, r).wait_recv()
        two = mid_y[j, x]
        for r in range(3):
            two = two + in_yx[j, r]
        for a in range(2):
            last[j, a, :, 0:256] = one[a * 8 : a * 8 + 8]
            last[j, a, :, 256:512] = two[a * 8 : a * 8 + 8]
        for a in range(2):
            @pl.when(z != 2 * j + a)
            def _():
                z_copy(j, a, lax.rem(z - (2 * j + a) + 8, 8) - 1).start()

    for g in range(4):
        normalise(g, 0)
    give.wait_recv()
    for g in range(4):
        normalise(g, 1)
        if g:
            turn_over(g - 1)
            weigh(0, (g - 1) * 640, 640)
    turn_over(3)
    weigh(0, 1920, 640)
    for j in range(1, CHUNKS + 1):
        for h in range(2):
            if j < CHUNKS:
                weigh(j, h * 1280, 640)
                weigh(j, h * 1280 + 640, 640)
            cross(j - 1, h)
        if j == CHUNKS:
            second(0)
        travel(j - 1)
    give.wait_send()
    for d in others:
        stat_copy(d).wait_send()
    for j in range(1, CHUNKS):
        second(j)
    for j in range(CHUNKS):
        for r in (1, 2, 3):
            x_copy(j, r).wait_send()
            y_copy(j, r).wait_send()
    for j in range(CHUNKS):
        third(j)

    for j in range(CHUNKS):
        for r in (1, 2, 3):
            xy_copy(j, r).wait_send()
            yx_copy(j, r).wait_send()
    for slot in range(7):
        z_copy(0, 0, slot).wait_recv()
    total = last[lax.div(z, 2), lax.rem(z, 2)]
    for slot in range(7):
        total = total + in_z[slot]
    at = pl.multiple_of((x * 4 + y) * 16 + lax.rem(z, 2) * 8, 8)
    out[...] = own_load[lax.div(z, 2), pl.ds(at, 8), :] * total / (tails * paths)

    for j in range(CHUNKS):
        for a in range(2):
            @pl.when(z != 2 * j + a)
            def _():
                z_copy(j, a, 0).wait_send()


def body(normals, states, loadings, strikes, hedge, sigma, tail):
    nodes, per_node, factors = normals.shape
    rows = CAP * per_node * 2
    dma = pltpu.SemaphoreType.DMA
    return pl.pallas_call(
        kernel,
        out_shape=pltpu.VMEM((8, factors), F32),
        in_specs=[pl.BlockSpec(memory_space=pltpu.HBM)] * 7,
        out_specs=pl.BlockSpec(memory_space=pltpu.VMEM),
        scratch_shapes=[
            pltpu.VMEM(normals.shape, BF16),
            pltpu.VMEM((CAP, per_node, factors), BF16),
            pltpu.VMEM((CAP, per_node, factors), BF16),
            pltpu.VMEM(loadings.shape, BF16),
            pltpu.VMEM(states.shape, BF16),
            pltpu.VMEM((4, nodes, 128), F32),
            pltpu.VMEM((8, 256), F32),
            pltpu.VMEM((8, 256), F32),
            pltpu.VMEM((1, factors), F32),
            pltpu.VMEM((4, 1, 128), F32),
            pltpu.SMEM(tail.shape, jnp.int32),
            pltpu.SMEM((CAP,), jnp.int32),
            pltpu.SMEM((CAP,), F32),
            pltpu.VMEM((2, 16, 5, 4, 128), F32),
            pltpu.VMEM((16, 5, 4, 128), F32),
            pltpu.VMEM((16, 5, 4, 128), F32),
            pltpu.VMEM((16, 5, 4, 128), F32),
            pltpu.VMEM((2, 16, 5, 4, 128), F32),
            pltpu.VMEM((CHUNKS, 1, 256), F32),
            pltpu.VMEM((CHUNKS, 1, 256), F32),
            pltpu.VMEM((CHUNKS, 256, factors), F32),
            pltpu.VMEM((CHUNKS, factors, 256), BF16),
            pltpu.VMEM((rows, factors), BF16),
            pltpu.VMEM((rows, factors), BF16),
            pltpu.VMEM((factors, rows), BF16),
            pltpu.VMEM((2, rows, 256), BF16),
            pltpu.VMEM((CHUNKS, 4, 4, 16, factors), BF16),
            pltpu.VMEM((CHUNKS, 3, 4, 16, 256), BF16),
            pltpu.VMEM((CHUNKS, 3, 4, 16, 256), BF16),
            pltpu.VMEM((CHUNKS, 4, 16, 256), F32),
            pltpu.VMEM((CHUNKS, 4, 16, 256), F32),
            pltpu.VMEM((CHUNKS, 3, 16, 256), F32),
            pltpu.VMEM((CHUNKS, 3, 16, 256), F32),
            pltpu.VMEM((CHUNKS, 2, 8, factors), F32),
            pltpu.VMEM((7, 8, factors), F32),
            dma((21,)),
            dma((2,)),
            dma((2,)),
            dma((2,)),
            dma((16,)),
            dma((16,)),
            dma((16,)),
            dma((16,)),
            dma((CHUNKS, 3)),
            dma((CHUNKS, 3)),
            dma((CHUNKS, 3)),
            dma((CHUNKS, 3)),
            dma((CHUNKS, 3)),
            dma((CHUNKS, 3)),
            dma((CHUNKS, 3)),
            dma((CHUNKS, 3)),
            dma((CHUNKS, 2)),
            dma((7,)),
        ],
        compiler_params=pltpu.CompilerParams(
            collective_id=0, has_side_effects=True, vmem_limit_bytes=63 * 1024 * 1024
        ),
    )(
        normals, states, loadings, strikes, hedge, sigma.reshape(1, factors), tail,
    )


def solution(mesh):
    in_specs = (P("outer", "inner", None), P("outer", None), P(), P(), P(), P(), P())
    out_specs = P(("outer", "inner"), None)
    return jax.shard_map(body, mesh=mesh, in_specs=in_specs, out_specs=out_specs, check_vma=False)
```

```python
import jax
import jax.numpy as jnp
from jax import lax
from jax.experimental import pallas as pl
from jax.experimental.pallas import tpu as pltpu
from jax.sharding import PartitionSpec as P

CAP = 80
EPSILON = 1e-06
CHUNKS = 4
MESH = pl.DeviceIdType.MESH
F32 = jnp.float32
BF16 = jnp.bfloat16


def place(hit):
    return jnp.where(hit, 1.0, 0.0)


def offsets():
    span = (0, 1, 2, 1)
    every = [(dx, dy) for dx in range(4) for dy in range(4)][1:]
    return sorted(every, key=lambda d: -(span[d[0]] + span[d[1]]))


def kernel(
    normals, states, loadings, strikes, hedge, sigma, tail, out,
    held, own, pair, load_v, states_b, states_f, strikes_v, hedge_v, sigma_v, sigma_f, tail_s, slot_s, live_s,
    sums, sums_pair, sums_chip, sums_in, stats, half_strike, half_hedge, own_load, load_t,
    mixed, part, turned, weight, sent, in_x, in_y, mid_x, mid_y, in_xy, in_yx, last, in_z,
    copy_sem, pair_sem, join_sem, pass_sem, sum_out, sum_in, stat_out, stat_in,
    x_out, x_in, y_out, y_in, xy_out, xy_in, yx_out, yx_in, z_out, z_in,
):
    z = lax.axis_index("outer")
    me = lax.axis_index("inner")
    x, y, c = lax.div(me, 8), lax.rem(lax.div(me, 2), 4), lax.rem(me, 2)
    nodes, per_node, factors = held.shape
    paths = per_node * 32
    tails = tail_s.shape[0]
    others = offsets()

    def device(dx, dy, dc):
        return (lax.rem(x + dx, 4) * 4 + lax.rem(y + dy, 4)) * 2 + lax.rem(c + dc, 2)

    copies = [
        (tail, tail_s), (normals, held), (states, states_b), (sigma, sigma_v), (loadings, load_v),
    ]
    for i in range(8):
        copies.append((strikes.at[pl.ds(i * 256, 256)], strikes_v.at[i]))
        copies.append((hedge.at[pl.ds(i * 256, 256)], hedge_v.at[i]))
    loads = [pltpu.make_async_copy(a, b, copy_sem.at[i]) for i, (a, b) in enumerate(copies)]
    loads[0].start()
    loads[1].start()

    barrier = pltpu.get_barrier_semaphore()

    def greet(where):
        pl.semaphore_signal(barrier, inc=1, device_id=where, device_id_type=MESH)

    for dx, dy in others:
        greet((z, device(dx, dy, 0)))
    for d in (4, 3, 5, 2, 6, 1, 7):
        greet((lax.rem(z + d, 8), me))
    partner = (z, device(0, 0, 1))
    greet(partner)
    loads[0].wait()
    first = jnp.int32(0)
    step = tails // 2
    while step:
        first = first + jnp.where(tail_s[first + step - 1] < z * nodes, step, 0)
        step //= 2

    def find(s, carry):
        at = jnp.minimum(first + s, tails - 1)
        node = tail_s[at] - z * nodes
        good = (first + s < tails) & (node >= 0) & (node < nodes)
        slot_s[s] = jnp.clip(node, 0, nodes - 1)
        live_s[s] = jnp.where(good, 1.0, 0.0).astype(F32)
        return carry

    lax.fori_loop(0, CAP, find, 0, unroll=8)
    loads[1].wait()
    for item in loads[2:]:
        item.start()

    def add_up(q, carry):
        for i in range(5):
            rows = held[slot_s[q * 5 + i]]
            own[q * 5 + i] = rows
            block = rows.astype(F32)
            one = jnp.sum(block, axis=0, keepdims=True)
            two = jnp.sum(block * block, axis=0, keepdims=True)
            for h in range(2):
                for b in range(2):
                    lanes = slice(h * 256 + b * 128, h * 256 + b * 128 + 128)
                    sums[h, q, i, b : b + 1, :] = one[:, lanes]
                    sums[h, q, i, 2 + b : 3 + b, :] = two[:, lanes]
        return carry

    lax.fori_loop(0, 16, add_up, 0)
    for item in loads[2:]:
        item.wait()
    for b in range(4):
        lanes = slice(b * 128, b * 128 + 128)
        states_f[b] = states_b[:, lanes].astype(F32)
        sigma_f[b] = sigma_v[:, lanes]
    pl.semaphore_wait(barrier, 23)

    join = pltpu.make_async_remote_copy(
        src_ref=sums.at[1 - c], dst_ref=sums_pair, send_sem=join_sem.at[0], recv_sem=join_sem.at[1],
        device_id=partner, device_id_type=MESH,
    )
    join.start()
    join.wait_recv()
    sums_chip[...] = sums[c] + sums_pair[...]

    def sum_copy(d):
        dx, dy = d
        return pltpu.make_async_remote_copy(
            src_ref=sums_chip.at[lax.rem(x + dx, 4) * 4 + lax.rem(y + dy, 4)],
            dst_ref=sums_in.at[dx * 4 + dy],
            send_sem=sum_out.at[dx * 4 + dy], recv_sem=sum_in.at[dx * 4 + dy],
            device_id=(z, device(dx, dy, 0)), device_id_type=MESH,
        )

    def stat_copy(d):
        dx, dy = d
        return pltpu.make_async_remote_copy(
            src_ref=stats.at[0, 0], dst_ref=stats.at[0, dx * 4 + dy],
            send_sem=stat_out.at[dx * 4 + dy], recv_sem=stat_in.at[dx * 4 + dy],
            device_id=(z, device(dx, dy, 0)), device_id_type=MESH,
        )

    for d in others:
        sum_copy(d).start()
    swap = pltpu.make_async_remote_copy(
        src_ref=own, dst_ref=pair, send_sem=pair_sem.at[0], recv_sem=pair_sem.at[1],
        device_id=partner, device_id_type=MESH,
    )
    swap.start()

    m_id = lax.broadcasted_iota(jnp.int32, (256, 256), 0)
    l_id = lax.broadcasted_iota(jnp.int32, (256, 256), 1)
    same = (m_id // 16 == l_id // 16) & (m_id % 8 == l_id % 8)
    picks = [same & ((m_id // 8) % 2 == c) & ((l_id // 8) % 2 == a) for a in range(2)]
    picks_t = [same & ((l_id // 8) % 2 == c) & ((m_id // 8) % 2 == a) for a in range(2)]
    for source, target in ((strikes_v, half_strike), (hedge_v, half_hedge)):
        rows = source[...] * 0.5
        moved = [
            jnp.dot(rows, place(pick), precision=lax.Precision.HIGHEST, preferred_element_type=F32)
            for pick in picks
        ]
        for j in range(CHUNKS):
            target[j] = moved[0][2 * j : 2 * j + 1] + moved[1][2 * j + 1 : 2 * j + 2]
    turn = [place(pick).astype(BF16) for pick in picks_t]

    def order(j, carry):
        rows = jnp.zeros((256, factors), F32)
        for a in range(2):
            at = pl.multiple_of((2 * j + a) * 256, 256)
            rows = rows + jnp.dot(turn[a], load_v[pl.ds(at, 256), :], preferred_element_type=F32)
        own_load[j] = rows
        load_t[j] = (rows * 0.5).astype(BF16).T
        return carry

    lax.fori_loop(0, CHUNKS, order, 0)

    total = sums_chip[x * 4 + y]
    for d in reversed(others):
        sum_copy(d).wait_recv()
        total = total + sums_in[d[0] * 4 + d[1]]
    center = total[:, 0:2, :] / paths
    spread = total[:, 2:4, :] / paths - center * center
    stats[0, 0, :, 0:2, :] = center
    stats[0, 0, :, 2:4, :] = lax.rsqrt(spread + EPSILON)
    for d in others:
        stat_copy(d).start()
    for d in others:
        sum_copy(d).wait_send()
    join.wait_send()
    swap.wait()
    for d in reversed(others):
        stat_copy(d).wait_recv()
    give = pltpu.make_async_remote_copy(
        src_ref=stats.at[0], dst_ref=stats.at[1], send_sem=pass_sem.at[0], recv_sem=pass_sem.at[1],
        device_id=partner, device_id_type=MESH,
    )
    give.start()

    def normalise(g, e):
        base = (c if e == 0 else 1 - c) * 2
        for dy in range(4):
            q = lax.rem(x + 4 - g, 4) * 4 + lax.rem(y + 4 - dy, 4)
            for i in range(5):
                s = q * 5 + i
                at, live = slot_s[s], live_s[s]
                for b in range(2):
                    lanes = pl.ds(pl.multiple_of((base + b) * 128, 128), 128)
                    state = states_f[base + b, pl.ds(at, 1), :]
                    mean = stats[e, g * 4 + dy, i, b : b + 1, :]
                    scale = stats[e, g * 4 + dy, i, 2 + b : 3 + b, :] * live
                    for w, source in enumerate((own, pair)):
                        row = (g * 4 + dy) * 160 + i * 32 + w * 16
                        block = source[s, :, lanes].astype(F32)
                        scaled = ((block - mean) * scale).astype(BF16)
                        both = state + sigma_f[base + b] * scaled.astype(F32)
                        mixed[row : row + 16, lanes] = both.astype(BF16)
                        part[row : row + 16, lanes] = scaled

    def turn_over(g):
        for b in range(5):
            at = g * 640 + b * 128
            turned[:, at : at + 128] = part[at : at + 128, :].T

    def weigh(j, at, count):
        level = jnp.dot(mixed[at : at + count, :], load_t[j], preferred_element_type=F32)
        size = half_hedge[j]
        fresh = size + size * jnp.tanh(level - half_strike[j])
        weight[j % 2, at : at + count, :] = fresh.astype(BF16)

    def x_copy(j, r):
        px = lax.rem(x + r, 4)
        return pltpu.make_async_remote_copy(
            src_ref=sent.at[j, px, :, :, pl.ds(0, 256)], dst_ref=in_x.at[j, r - 1],
            send_sem=x_out.at[j, r - 1], recv_sem=x_in.at[j, r - 1],
            device_id=(z, device(r, 0, 0)), device_id_type=MESH,
        )

    def y_copy(j, r):
        py = lax.rem(y + r, 4)
        return pltpu.make_async_remote_copy(
            src_ref=sent.at[j, :, py, :, pl.ds(256, 256)], dst_ref=in_y.at[j, r - 1],
            send_sem=y_out.at[j, r - 1], recv_sem=y_in.at[j, r - 1],
            device_id=(z, device(0, r, 0)), device_id_type=MESH,
        )

    def xy_copy(j, r):
        py = lax.rem(y + r, 4)
        return pltpu.make_async_remote_copy(
            src_ref=mid_x.at[j, py], dst_ref=in_xy.at[j, r - 1],
            send_sem=xy_out.at[j, r - 1], recv_sem=xy_in.at[j, r - 1],
            device_id=(z, device(0, r, 0)), device_id_type=MESH,
        )

    def yx_copy(j, r):
        px = lax.rem(x + r, 4)
        return pltpu.make_async_remote_copy(
            src_ref=mid_y.at[j, px], dst_ref=in_yx.at[j, r - 1],
            send_sem=yx_out.at[j, r - 1], recv_sem=yx_in.at[j, r - 1],
            device_id=(z, device(r, 0, 0)), device_id_type=MESH,
        )

    def z_copy(j, a, slot):
        return pltpu.make_async_remote_copy(
            src_ref=last.at[j, a], dst_ref=in_z.at[slot],
            send_sem=z_out.at[j, a], recv_sem=z_in.at[slot],
            device_id=(2 * j + a, me), device_id_type=MESH,
        )

    def cross(j, h):
        at = h * 256
        rows = jnp.dot(turned[at : at + 256, :], weight[j % 2], preferred_element_type=F32)
        sent[j, :, :, :, at : at + 256] = rows.astype(BF16).T.reshape(4, 4, 16, 256)

    def travel(j):
        for r in (2, 1, 3):
            x_copy(j, r).start()
            y_copy(j, r).start()

    def second(j):
        for r in (1, 3, 2):
            x_copy(j, r).wait_recv()
        total = sent[j, x, :, :, 0:256].astype(F32)
        for r in range(3):
            total = total + in_x[j, r].astype(F32)
        mid_x[j] = total
        for r in (1, 3, 2):
            y_copy(j, r).wait_recv()
        for r in (2, 1, 3):
            xy_copy(j, r).start()
        total = sent[j, :, y, :, 256:512].astype(F32)
        for r in range(3):
            total = total + in_y[j, r].astype(F32)
        mid_y[j] = total
        for r in (2, 1, 3):
            yx_copy(j, r).start()

    def third(j):
        for r in (1, 3, 2):
            xy_copy(j, r).wait_recv()
        one = mid_x[j, y]
        for r in range(3):
            one = one + in_xy[j, r]
        for r in (1, 3, 2):
            yx_copy(j, r).wait_recv()
        two = mid_y[j, x]
        for r in range(3):
            two = two + in_yx[j, r]
        for a in range(2):
            last[j, a, :, 0:256] = one[a * 8 : a * 8 + 8]
            last[j, a, :, 256:512] = two[a * 8 : a * 8 + 8]
        for a in range(2):
            @pl.when(z != 2 * j + a)
            def _():
                z_copy(j, a, lax.rem(z - (2 * j + a) + 8, 8) - 1).start()

    for g in range(4):
        normalise(g, 0)
    give.wait_recv()
    for g in range(4):
        normalise(g, 1)
        if g:
            turn_over(g - 1)
            weigh(0, (g - 1) * 640, 640)
    turn_over(3)
    weigh(0, 1920, 640)
    for j in range(1, CHUNKS + 1):
        for h in range(2):
            if j < CHUNKS:
                weigh(j, h * 1280, 640)
                weigh(j, h * 1280 + 640, 640)
            cross(j - 1, h)
        if j == CHUNKS:
            second(0)
        travel(j - 1)
    give.wait_send()
    for d in others:
        stat_copy(d).wait_send()
    for j in range(1, CHUNKS):
        second(j)
    for j in range(CHUNKS):
        for r in (1, 2, 3):
            x_copy(j, r).wait_send()
            y_copy(j, r).wait_send()
    for j in range(CHUNKS):
        third(j)

    for j in range(CHUNKS):
        for r in (1, 2, 3):
            xy_copy(j, r).wait_send()
            yx_copy(j, r).wait_send()
    for slot in range(7):
        z_copy(0, 0, slot).wait_recv()
    total = last[lax.div(z, 2), lax.rem(z, 2)]
    for slot in range(7):
        total = total + in_z[slot]
    at = pl.multiple_of((x * 4 + y) * 16 + lax.rem(z, 2) * 8, 8)
    out[...] = own_load[lax.div(z, 2), pl.ds(at, 8), :] * total / (tails * paths)

    for j in range(CHUNKS):
        for a in range(2):
            @pl.when(z != 2 * j + a)
            def _():
                z_copy(j, a, 0).wait_send()


def body(normals, states, loadings, strikes, hedge, sigma, tail):
    nodes, per_node, factors = normals.shape
    rows = CAP * per_node * 2
    dma = pltpu.SemaphoreType.DMA
    return pl.pallas_call(
        kernel,
        out_shape=pltpu.VMEM((8, factors), F32),
        in_specs=[pl.BlockSpec(memory_space=pltpu.HBM)] * 7,
        out_specs=pl.BlockSpec(memory_space=pltpu.VMEM),
        scratch_shapes=[
            pltpu.VMEM(normals.shape, BF16),
            pltpu.VMEM((CAP, per_node, factors), BF16),
            pltpu.VMEM((CAP, per_node, factors), BF16),
            pltpu.VMEM(loadings.shape, BF16),
            pltpu.VMEM(states.shape, BF16),
            pltpu.VMEM((4, nodes, 128), F32),
            pltpu.VMEM((8, 256), F32),
            pltpu.VMEM((8, 256), F32),
            pltpu.VMEM((1, factors), F32),
            pltpu.VMEM((4, 1, 128), F32),
            pltpu.SMEM(tail.shape, jnp.int32),
            pltpu.SMEM((CAP,), jnp.int32),
            pltpu.SMEM((CAP,), F32),
            pltpu.VMEM((2, 16, 5, 4, 128), F32),
            pltpu.VMEM((16, 5, 4, 128), F32),
            pltpu.VMEM((16, 5, 4, 128), F32),
            pltpu.VMEM((16, 5, 4, 128), F32),
            pltpu.VMEM((2, 16, 5, 4, 128), F32),
            pltpu.VMEM((CHUNKS, 1, 256), F32),
            pltpu.VMEM((CHUNKS, 1, 256), F32),
            pltpu.VMEM((CHUNKS, 256, factors), F32),
            pltpu.VMEM((CHUNKS, factors, 256), BF16),
            pltpu.VMEM((rows, factors), BF16),
            pltpu.VMEM((rows, factors), BF16),
            pltpu.VMEM((factors, rows), BF16),
            pltpu.VMEM((2, rows, 256), BF16),
            pltpu.VMEM((CHUNKS, 4, 4, 16, factors), BF16),
            pltpu.VMEM((CHUNKS, 3, 4, 16, 256), BF16),
            pltpu.VMEM((CHUNKS, 3, 4, 16, 256), BF16),
            pltpu.VMEM((CHUNKS, 4, 16, 256), F32),
            pltpu.VMEM((CHUNKS, 4, 16, 256), F32),
            pltpu.VMEM((CHUNKS, 3, 16, 256), F32),
            pltpu.VMEM((CHUNKS, 3, 16, 256), F32),
            pltpu.VMEM((CHUNKS, 2, 8, factors), F32),
            pltpu.VMEM((7, 8, factors), F32),
            dma((21,)),
            dma((2,)),
            dma((2,)),
            dma((2,)),
            dma((16,)),
            dma((16,)),
            dma((16,)),
            dma((16,)),
            dma((CHUNKS, 3)),
            dma((CHUNKS, 3)),
            dma((CHUNKS, 3)),
            dma((CHUNKS, 3)),
            dma((CHUNKS, 3)),
            dma((CHUNKS, 3)),
            dma((CHUNKS, 3)),
            dma((CHUNKS, 3)),
            dma((CHUNKS, 2)),
            dma((7,)),
        ],
        compiler_params=pltpu.CompilerParams(
            collective_id=0, has_side_effects=True, vmem_limit_bytes=63 * 1024 * 1024
        ),
    )(
        normals, states, loadings, strikes, hedge, sigma.reshape(1, factors), tail,
    )


def solution(mesh):
    in_specs = (P("outer", "inner", None), P("outer", None), P(), P(), P(), P(), P())
    out_specs = P(("outer", "inner"), None)
    return jax.shard_map(body, mesh=mesh, in_specs=in_specs, out_specs=out_specs, check_vma=False)
```
